128 devices in a mesh: span: 32 (over y, x, core), head: 4 (over z).
Axes of the slice: x: 4, y: 4, z: 4, core: 2. Of those that a mesh axis runs over, the one named last changes fastest.
Arguments:
- neighbour_query: bfloat16 [32768, 4096], P('span', 'head'), may hold values from -12 to 12
- neighbour_key: bfloat16 [32768, 4096], P('span', 'head'), may hold values from -6 to 6
- neighbour_value: bfloat16 [32768, 4096], P('span', 'head'), may hold values from -12.2 to 12.2
- segment_key: bfloat16 [8192, 4096], P('span', 'head'), may hold values from -30 to 30
- segment_value: bfloat16 [8192, 4096], P('span', 'head'), may hold values from -6 to 6
- decoder_query: bfloat16 [8192, 4096], P('span', 'head'), may hold values from -24 to 24
- sources: int32 [128, 2], P('span'), may hold values from 0 to 127, as said below
Outputs:
- blended: bfloat16 [8192, 4096], P('span', 'head')
The draws below stay inside these ranges and needn't reach their ends.
Inputs may be any that keep to these rules, and one draw needn't show every extreme that they name: `sources`: the segments of index o of span are o * 4 to (o + 1) * 4 - 1. Among the 8 entries of the segments of one index of span, at most 2 name segments of one index of span, and in every such block some index is named exactly 2 times.
All inputs are finite; a program needn't handle non-finite values.
Results may differ from the reference program's by a relative error of at most 0.035.
Values may be sent and summed in bfloat16 or wider, within the bound.
No kernel may reach another device: no remote copies, remote signals or barrier semaphores. Data moves between devices by JAX's collectives and lax.ppermute only.
A program may use at most 192 MiB of HBM per device.

```python
import math
import jax
import jax.numpy as jnp
from jax import lax

HEAD_DIM = 128
SEG_LEN = 64
NBR_LEN = 128
NEIGHBOURS = 2
SEG_DEV = 4
HIDDEN_COLS = 4096
SEGMENTS = 128
CAPACITY = 2
N_SPAN = 32


def rising_scales():
    return 0.3 * jnp.exp(math.log(10.0) * jnp.arange(HIDDEN_COLS, dtype=jnp.float32) / HIDDEN_COLS)


def draw_sources(key, part):
    keys = jax.random.split(jax.random.fold_in(key, 26), 5)
    per_block = SEG_DEV * NEIGHBOURS
    slot_count_total = N_SPAN * CAPACITY
    favoured_rows = jax.random.randint(keys[0], (N_SPAN,), 0, 4)
    slot_holder_index = jnp.arange(slot_count_total) // CAPACITY
    random_jitter = jax.random.randint(keys[1], (N_SPAN, slot_count_total), 0, 1024)
    hotspot_row = jax.random.randint(keys[2], (N_SPAN,), 0, N_SPAN)
    extra_score = jnp.where(slot_holder_index[None, :] == hotspot_row[:, None], 8, 0)
    logit_scores = ((favoured_rows[slot_holder_index][None, :] + extra_score) * 1024 + random_jitter) * slot_count_total + jnp.arange(slot_count_total)[None, :]
    top_values, top_index = lax.top_k(logit_scores, per_block)
    owners = slot_holder_index[top_index]
    mixing = jax.random.randint(keys[3], (N_SPAN, per_block), 0, 1 << 20) * per_block + jnp.arange(per_block)[None, :]
    shuffle = jnp.argsort(mixing, axis=1)
    owners = jnp.take_along_axis(owners, shuffle, axis=1)
    within = jax.random.randint(keys[4], (N_SPAN, per_block), 0, SEG_DEV)
    return (owners * SEG_DEV + within).reshape(SEGMENTS, NEIGHBOURS).astype(jnp.int32)


def draw_neighbour_query(key, part):
    row_total = SEGMENTS * NEIGHBOURS * NBR_LEN
    sample_key = jax.random.fold_in(key, 21)
    return jnp.clip(2.0 * jax.random.normal(sample_key, (row_total, HIDDEN_COLS), jnp.float32), -12.0, 12.0).astype(jnp.bfloat16)


def draw_neighbour_key(key, part):
    row_total = SEGMENTS * NEIGHBOURS * NBR_LEN
    sample_key = jax.random.fold_in(key, 22)
    return jnp.clip(jax.random.normal(sample_key, (row_total, HIDDEN_COLS), jnp.float32), -6.0, 6.0).astype(jnp.bfloat16)


def draw_neighbour_value(key, part):
    row_total = SEGMENTS * NEIGHBOURS * NBR_LEN
    sample_key = jax.random.fold_in(key, 23)
    filler = jnp.clip(jax.random.normal(sample_key, (row_total, HIDDEN_COLS), jnp.float32), -4.0, 4.0)
    return (filler * rising_scales()[None, :]).astype(jnp.bfloat16)


def draw_segment_key(key, part):
    row_total = SEGMENTS * SEG_LEN
    sample_key = jax.random.fold_in(key, 24)
    return jnp.clip(2.0 * jax.random.normal(sample_key, (row_total, HIDDEN_COLS), jnp.float32), -12.0, 12.0).astype(jnp.bfloat16)


def draw_decoder_query(key, part):
    row_total = SEGMENTS * SEG_LEN
    sample_key = jax.random.fold_in(key, 25)
    return jnp.clip(3.0 * jax.random.normal(sample_key, (row_total, HIDDEN_COLS), jnp.float32), -18.0, 18.0).astype(jnp.bfloat16)


def block_levels(rng, extent, pieces, low, high):
    loudness = 1.0
    for dim, shards_of in pieces:
        draws = jax.random.uniform(jax.random.fold_in(jax.random.fold_in(rng, 6), dim), (shards_of,), jnp.float32, low / len(pieces), high / len(pieces))
        loudness = loudness * jnp.repeat(jnp.exp(draws), extent[dim] // shards_of).reshape((-1,) + (1,) * (len(extent) - 1 - dim))
    return loudness


def normal_values(key, extent, spread, most, cuts=(), held_as=jnp.bfloat16):
    values = jax.random.normal(key, extent, jnp.float32) * spread
    if len(cuts) > 0:
        values = block_levels(key, extent, cuts, -0.22, 0.18) * values
    return jnp.clip(values, min=-most, max=most).astype(held_as)


def setup_inputs(seed: int = 0) -> dict:
    seeds = jax.random.split(jax.random.key(seed), 8)
    neighbour_query = draw_neighbour_query(jax.random.fold_in(seeds[7], 71), 0)
    neighbour_key = draw_neighbour_key(jax.random.fold_in(seeds[7], 71), 0)
    neighbour_value = draw_neighbour_value(jax.random.fold_in(seeds[7], 71), 0)
    segment_key = draw_segment_key(jax.random.fold_in(seeds[7], 71), 0)
    segment_value = normal_values(seeds[4], (SEGMENTS * SEG_LEN, HIDDEN_COLS), 1.0, 6.0, ((0, 32), (1, 4)))
    decoder_query = draw_decoder_query(jax.random.fold_in(seeds[7], 71), 0)
    sources = draw_sources(jax.random.fold_in(seeds[7], 71), 0)
    return {"neighbour_query": neighbour_query, "neighbour_key": neighbour_key, "neighbour_value": neighbour_value, "segment_key": segment_key, "segment_value": segment_value, "decoder_query": decoder_query, "sources": sources}


epsilon = 1e-06

def attend(query_rows, key_rows, value_rows):
    groups, length, columns = query_rows.shape
    head_count = columns // HEAD_DIM
    query_heads = query_rows.astype(jnp.float32).reshape(groups, length, head_count, HEAD_DIM)
    key_heads = key_rows.astype(jnp.float32).reshape(groups, key_rows.shape[1], head_count, HEAD_DIM)
    value_heads = value_rows.astype(jnp.float32).reshape(groups, value_rows.shape[1], head_count, HEAD_DIM)
    logit_scores = jnp.einsum('bqhd,bkhd->bhqk', query_heads, key_heads) * HEAD_DIM ** (-0.5)
    logit_scores = logit_scores - lax.optimization_barrier(jnp.max(logit_scores, axis=-1, keepdims=True))
    weights = jnp.exp(logit_scores)
    weights = (weights / lax.optimization_barrier(jnp.sum(weights, axis=-1, keepdims=True))).astype(jnp.bfloat16)
    output = jnp.einsum('bhqk,bkhd->bqhd', weights.astype(jnp.float32), value_heads)
    return output.reshape(groups, length, columns)

def normalize(rows):
    wide = rows.astype(jnp.float32)
    meansq = lax.optimization_barrier(jnp.mean(wide * wide, axis=-1, keepdims=True))
    return (wide * lax.rsqrt(meansq + epsilon)).astype(jnp.bfloat16)

def reference(neighbour_query, neighbour_key, neighbour_value, segment_key, segment_value, decoder_query, sources):
    columns = neighbour_query.shape[1]
    per_device = SEG_DEV * NEIGHBOURS
    all_keys = segment_key.reshape(SEGMENTS, SEG_LEN, columns)
    all_values = segment_value.reshape(SEGMENTS, SEG_LEN, columns)

    def encode(group):
        query_rows, key_rows, value_rows, listed = group
        self_out = attend(query_rows, key_rows, value_rows).astype(jnp.bfloat16)
        cross_query = normalize(self_out)
        crossed = attend(cross_query, all_keys[listed], all_values[listed]).astype(jnp.bfloat16)
        return (self_out.astype(jnp.float32) + crossed.astype(jnp.float32)).astype(jnp.bfloat16)

    def shaped(array):
        return array.reshape(N_SPAN, per_device, NBR_LEN, columns)
    listed_all = sources.reshape(N_SPAN, per_device).astype(jnp.int32)
    encoded = lax.map(encode, (shaped(neighbour_query), shaped(neighbour_key), shaped(neighbour_value), listed_all))
    encoded = encoded.reshape(SEGMENTS, NEIGHBOURS * NBR_LEN, columns)
    prior = jnp.concatenate([jnp.zeros((1, NEIGHBOURS * NBR_LEN, columns), jnp.bfloat16), encoded[:-1]], axis=0)

    def decode(group):
        query_rows, value_rows = group
        return attend(query_rows, normalize(value_rows), value_rows).astype(jnp.bfloat16)
    blended = lax.map(decode, (decoder_query.reshape(N_SPAN, SEG_DEV, SEG_LEN, columns), prior.reshape(N_SPAN, SEG_DEV, NEIGHBOURS * NBR_LEN, columns)))
    return blended.reshape(SEGMENTS * SEG_LEN, columns)
```

```python
import functools

import jax
import jax.numpy as jnp
from jax import lax
from jax.experimental import pallas as pl
from jax.experimental.pallas import tpu as pltpu
from jax.sharding import PartitionSpec as P

HEAD_DIM = 128
SEG_LEN = 64
NBR_LEN = 128
NEIGHBOURS = 2
SEG_DEV = 4

EPSILON = 1e-06
LOG2E = 1.4426950408889634
SCALE2 = HEAD_DIM ** (-0.5) * LOG2E
HALF = SEG_LEN // 2
TAIL = 8

F32 = jnp.float32
BF16 = jnp.bfloat16


def dot(a, b, contract):
    return lax.dot_general(a, b, ((contract[:1], contract[1:]), ((), ())), preferred_element_type=F32)


def cost(flops, moved, exps=0):
    return pl.CostEstimate(flops=flops, bytes_accessed=moved, transcendentals=exps)


def params(**more):
    return pltpu.CompilerParams(vmem_limit_bytes=40 * 1024 * 1024, **more)


def pack_kernel(sources_ref, key_ref, value_ref, out_ref):
    heads = key_ref.shape[1] // HEAD_DIM
    listed = SEG_DEV * NEIGHBOURS
    lane = lax.broadcasted_iota(jnp.int32, (TAIL, HEAD_DIM), 1)
    tail = jnp.zeros((TAIL, HEAD_DIM), F32)
    for i in range(listed):
        named = sources_ref[i // NEIGHBOURS, i % NEIGHBOURS].astype(F32)
        tail = jnp.where(lane == i, named, tail)
    tail = tail.astype(BF16)
    for kv, ref in enumerate((key_ref, value_ref)):
        for half in range(2):
            for head in range(heads):
                stripe = (kv * 2 + half) * heads + head
                for seg in range(SEG_DEV):
                    row = seg * SEG_LEN + half * HALF
                    out_ref[stripe, seg * HALF:(seg + 1) * HALF, :] = ref[
                        row:row + HALF, head * HEAD_DIM:(head + 1) * HEAD_DIM
                    ]
                out_ref[stripe, SEG_DEV * HALF:SEG_DEV * HALF + TAIL, :] = tail


def pack(sources, segment_key, segment_value):
    columns = segment_key.shape[1]
    stripes = 4 * columns // HEAD_DIM
    shape = (stripes, SEG_DEV * HALF + TAIL, HEAD_DIM)
    return pl.pallas_call(
        pack_kernel,
        out_shape=jax.ShapeDtypeStruct(shape, BF16),
        in_specs=[
            pl.BlockSpec(memory_space=pltpu.SMEM),
            pl.BlockSpec(memory_space=pltpu.VMEM),
            pl.BlockSpec(memory_space=pltpu.VMEM),
        ],
        out_specs=pl.BlockSpec(memory_space=pltpu.VMEM),
        compiler_params=params(),
        cost_estimate=cost(1000000, 2 * 2 * segment_key.size * 2),
        name="pack_stripes",
    )(sources, segment_key, segment_value)


def pick_kernel(first, count, table_sources_ref, table_ref, out_ref):
    devices = out_ref.shape[0]

    def one(device, carry):
        for i in range(count):
            named = table_sources_ref[device, first + i]
            owner = lax.shift_right_logical(named, 2)
            within = lax.bitwise_and(named, SEG_DEV - 1)
            start = pl.multiple_of(within * HALF, HALF)
            out_ref[device, i * HALF:(i + 1) * HALF, :] = table_ref[owner, pl.ds(start, HALF), :]
        return carry

    lax.fori_loop(0, devices, one, 0)


def pick(named, table, first, count):
    devices = table.shape[0]
    return pl.pallas_call(
        functools.partial(pick_kernel, first, count),
        out_shape=jax.ShapeDtypeStruct((devices, count * HALF, HEAD_DIM), BF16),
        in_specs=[pl.BlockSpec(memory_space=pltpu.SMEM), pl.BlockSpec(memory_space=pltpu.VMEM)],
        out_specs=pl.BlockSpec(memory_space=pltpu.VMEM),
        compiler_params=params(),
        cost_estimate=cost(1000000, 2 * table.size + 2 * devices * count * HALF * HEAD_DIM),
        name="pick_stripes",
    )(named, table)


def lanes_of(square):
    return jnp.sum(square.T, axis=0, keepdims=True)


def self_kernel(query_ref, key_ref, value_ref, out_ref, squares_ref):
    n = pl.program_id(0)
    total = jnp.zeros((NBR_LEN, HEAD_DIM), F32)
    for head in range(query_ref.shape[1] // HEAD_DIM):
        at = slice(head * HEAD_DIM, (head + 1) * HEAD_DIM)
        scores = dot(key_ref[:, at], query_ref[:, at], (1, 1))
        top = jnp.max(scores, axis=0, keepdims=True)
        weights = jnp.exp2((scores - top) * SCALE2)
        weights = weights * (1.0 / jnp.sum(weights, axis=0, keepdims=True))
        rows = dot(weights.astype(BF16), value_ref[:, at], (0, 0)).astype(BF16)
        out_ref[:, at] = rows
        wide = rows.astype(F32)
        total = total + wide * wide
    squares_ref[pl.ds(n, 1), :] = lanes_of(total)


def self_attention(query, key, value):
    rows, columns = query.shape
    count = rows // NBR_LEN
    block = pl.BlockSpec((NBR_LEN, columns), lambda n: (n, 0))
    return pl.pallas_call(
        self_kernel,
        grid=(count,),
        out_shape=(
            jax.ShapeDtypeStruct((rows, columns), BF16),
            jax.ShapeDtypeStruct((count, NBR_LEN), F32),
        ),
        in_specs=[block, block, block],
        out_specs=(block, pl.BlockSpec((count, NBR_LEN), lambda n: (0, 0))),
        compiler_params=params(),
        cost_estimate=cost(4 * rows * NBR_LEN * columns, 8 * rows * columns, rows * columns),
        name="self_attention",
    )(query, key, value)


def cross_kernel(first, full_width, self_ref, got_ref, totals_ref, out_ref, squares_ref):
    n = pl.program_id(0)
    heads = self_ref.shape[1] // HEAD_DIM
    scale = lax.rsqrt(totals_ref[pl.ds(first + n, 1), :] / full_width + EPSILON) * SCALE2
    total = jnp.zeros((NBR_LEN, HEAD_DIM), F32)
    for head in range(heads):
        at = slice(head * HEAD_DIM, (head + 1) * HEAD_DIM)
        own = self_ref[:, at]
        key = jnp.concatenate([got_ref[head], got_ref[heads + head]], axis=0)
        value = jnp.concatenate([got_ref[2 * heads + head], got_ref[3 * heads + head]], axis=0)
        scores = dot(key, own, (1, 1))
        top = jnp.max(scores, axis=0, keepdims=True)
        weights = jnp.exp2((scores - top) * scale)
        weights = weights * (1.0 / jnp.sum(weights, axis=0, keepdims=True))
        crossed = dot(weights.astype(BF16), value, (0, 0)).astype(BF16)
        rows = (own.astype(F32) + crossed.astype(F32)).astype(BF16)
        out_ref[:, at] = rows
        wide = rows.astype(F32)
        total = total + wide * wide
    squares_ref[pl.ds(n, 1), :] = lanes_of(total)


def cross_attention(self_out, got, totals, first, count, got_first, full_width):
    columns = self_out.shape[1]
    rows = count * NBR_LEN
    return pl.pallas_call(
        functools.partial(cross_kernel, first, full_width),
        grid=(count,),
        out_shape=(
            jax.ShapeDtypeStruct((rows, columns), BF16),
            jax.ShapeDtypeStruct((count, NBR_LEN), F32),
        ),
        in_specs=[
            pl.BlockSpec((NBR_LEN, columns), lambda n: (first + n, 0)),
            pl.BlockSpec((got.shape[0], HALF, HEAD_DIM), lambda n: (0, got_first + n, 0)),
            pl.BlockSpec(totals.shape, lambda n: (0, 0)),
        ],
        out_specs=(
            pl.BlockSpec((NBR_LEN, columns), lambda n: (n, 0)),
            pl.BlockSpec((count, NBR_LEN), lambda n: (0, 0)),
        ),
        compiler_params=params(),
        cost_estimate=cost(4 * rows * SEG_LEN * columns, 6 * rows * columns, rows * columns // 2),
        name="cross_attention",
    )(self_out, got, totals)


def decode_kernel(full_width, *refs):
    query_ref, prior_ref, totals_ref, out_ref = refs[-4:]
    u = pl.program_id(0)
    scale = lax.rsqrt(totals_ref[u] / full_width + EPSILON) * SCALE2
    for head in range(query_ref.shape[1] // HEAD_DIM):
        at = slice(head * HEAD_DIM, (head + 1) * HEAD_DIM)
        prior = prior_ref[:, at]
        scores = dot(query_ref[:, at], prior, (1, 1)) * scale
        top = jnp.max(scores, axis=1, keepdims=True)
        weights = jnp.exp2(scores - top)
        weights = weights * (1.0 / jnp.sum(weights, axis=1, keepdims=True))
        out_ref[:, at] = dot(weights.astype(BF16), prior, (1, 0)).astype(BF16)


def decode(query, prior, totals, first, held, full_width):
    columns = query.shape[1]
    panel = NEIGHBOURS * NBR_LEN
    count = prior.shape[0] // panel
    query_block = pl.BlockSpec((SEG_LEN, columns), lambda u: (first + u, 0))
    in_specs = [
        query_block,
        pl.BlockSpec((panel, columns), lambda u: (u, 0)),
        pl.BlockSpec((count, 1, panel), lambda u: (0, 0, 0)),
    ]
    operands = (query, prior, totals.reshape(count, 1, panel))
    aliases = {}
    if held is not None:
        in_specs = [pl.BlockSpec(memory_space=pl.ANY)] + in_specs
        operands = (held,) + operands
        aliases = {0: 0}
    rows = count * SEG_LEN
    return pl.pallas_call(
        functools.partial(decode_kernel, full_width),
        grid=(count,),
        out_shape=jax.ShapeDtypeStruct(query.shape, BF16),
        in_specs=in_specs,
        out_specs=query_block,
        input_output_aliases=aliases,
        compiler_params=params(),
        cost_estimate=cost(4 * rows * panel * columns, 4 * rows * columns + 2 * prior.size, rows * 2 * columns),
        name="decode",
    )(*operands)


def over_heads(part):
    heads = lax.axis_size("head")
    total = part
    for step in range(1, heads):
        total = total + lax.ppermute(part, "head", [(i, (i + step) % heads) for i in range(heads)])
    return total


def from_behind(part):
    devices = lax.axis_size("span")
    return lax.ppermute(part, "span", [(i, i + 1) for i in range(devices - 1)])


def total_from_behind(part):
    devices, heads = lax.axis_size("span"), lax.axis_size("head")
    total = None
    for step in range(heads):
        pairs = [
            (s * heads + h, (s + 1) * heads + (h + step) % heads)
            for s in range(devices - 1)
            for h in range(heads)
        ]
        came = lax.ppermute(part, ("span", "head"), pairs)
        total = came if total is None else total + came
    return total


def exchange(x):
    return lax.all_to_all(x, "span", split_axis=0, concat_axis=0, tiled=True)


def body(
    neighbour_query,
    neighbour_key,
    neighbour_value,
    segment_key,
    segment_value,
    decoder_query,
    sources,
):
    columns = neighbour_query.shape[1]
    full_width = columns * lax.axis_size("head")
    per_device = SEG_DEV * NEIGHBOURS
    table = exchange(pack(sources, segment_key, segment_value))
    self_out, squares = self_attention(neighbour_query, neighbour_key, neighbour_value)
    totals = over_heads(squares)
    named = table[:, SEG_DEV * HALF, :per_device].astype(jnp.int32)
    got = exchange(pick(named, table, 0, per_device))
    last = per_device - NEIGHBOURS
    panel, panel_squares = cross_attention(self_out, got, totals, last, NEIGHBOURS, last, full_width)
    came = from_behind(panel)
    came_totals = total_from_behind(panel_squares)
    rest, rest_squares = cross_attention(self_out, got, totals, 0, last, 0, full_width)
    rest_totals = over_heads(rest_squares)
    blended = decode(decoder_query, rest, rest_totals, 1, None, full_width)
    return decode(decoder_query, came, came_totals, 0, blended, full_width)


def solution(mesh):
    placed = (
        P("span", "head"),
        P("span", "head"),
        P("span", "head"),
        P("span", "head"),
        P("span", "head"),
        P("span", "head"),
        P("span", None),
    )
    return jax.shard_map(
        body, mesh=mesh, in_specs=placed, out_specs=P("span", "head"), check_vma=False
    )
```

```python
import functools

import jax
import jax.numpy as jnp
from jax import lax
from jax.experimental import pallas as pl
from jax.experimental.pallas import tpu as pltpu
from jax.sharding import PartitionSpec as P

HEAD_DIM = 128
SEG_LEN = 64
NBR_LEN = 128
NEIGHBOURS = 2
SEG_DEV = 4

EPSILON = 1e-06
LOG2E = 1.4426950408889634
SCALE2 = HEAD_DIM ** (-0.5) * LOG2E
HALF = SEG_LEN // 2
TAIL = 8
PACK_MIB = 60
SELF_MIB = 60
SMALL_MIB = 24

F32 = jnp.float32
BF16 = jnp.bfloat16


def dot(a, b, contract):
    return lax.dot_general(a, b, ((contract[:1], contract[1:]), ((), ())), preferred_element_type=F32)


def cost(flops, moved, exps=0):
    return pl.CostEstimate(flops=flops, bytes_accessed=moved, transcendentals=exps)


def params(mib):
    return pltpu.CompilerParams(vmem_limit_bytes=mib * 1024 * 1024)


def pack_kernel(sources_ref, key_ref, value_ref, out_ref):
    heads = key_ref.shape[1] // HEAD_DIM
    lane = lax.broadcasted_iota(jnp.int32, (TAIL, HEAD_DIM), 1)
    tail = jnp.zeros((TAIL, HEAD_DIM), F32)
    for i in range(SEG_DEV * NEIGHBOURS):
        named = sources_ref[i % NEIGHBOURS, i // NEIGHBOURS].astype(F32)
        tail = jnp.where(lane == i, named, tail)
    tail = tail.astype(BF16)
    for kv, ref in enumerate((key_ref, value_ref)):
        for half in range(2):
            for head in range(heads):
                for seg in range(SEG_DEV):
                    row = seg * SEG_LEN + half * HALF
                    out_ref[kv * 2 + half, head, seg * HALF:(seg + 1) * HALF, :] = ref[
                        row:row + HALF, head * HEAD_DIM:(head + 1) * HEAD_DIM
                    ]
                out_ref[kv * 2 + half, head, SEG_DEV * HALF:SEG_DEV * HALF + TAIL, :] = tail


def pack(sources, segment_key, segment_value):
    rows, columns = segment_key.shape
    heads = columns // HEAD_DIM
    long = SEG_DEV * HALF + TAIL
    steps = 4
    block = pl.BlockSpec((rows, columns // steps), lambda i: (0, i))
    out = pl.pallas_call(
        pack_kernel,
        grid=(steps,),
        out_shape=jax.ShapeDtypeStruct((4, heads, long, HEAD_DIM), BF16),
        in_specs=[pl.BlockSpec(memory_space=pltpu.SMEM), block, block],
        out_specs=pl.BlockSpec((4, heads // steps, long, HEAD_DIM), lambda i: (0, i, 0, 0)),
        compiler_params=params(PACK_MIB),
        cost_estimate=cost(1000000, 2 * 2 * segment_key.size * 2),
        name="pack_stripes",
    )(sources.T, segment_key, segment_value)
    return out.reshape(4 * heads, long, HEAD_DIM)


def pick_kernel(named_ref, table_ref, out_ref):
    devices = out_ref.shape[0]
    count = SEG_DEV * NEIGHBOURS

    def one(device, carry):
        for i in range(count):
            named = named_ref[device, i]
            owner = lax.shift_right_logical(named, 2)
            within = lax.bitwise_and(named, SEG_DEV - 1)
            start = pl.multiple_of(within * HALF, HALF)
            out_ref[device, i * HALF:(i + 1) * HALF, :] = table_ref[owner, pl.ds(start, HALF), :]
        return carry

    lax.fori_loop(0, devices, one, 0, unroll=2)


def pick(named, table):
    devices = table.shape[0]
    count = SEG_DEV * NEIGHBOURS
    return pl.pallas_call(
        pick_kernel,
        out_shape=jax.ShapeDtypeStruct((devices, count * HALF, HEAD_DIM), BF16),
        in_specs=[pl.BlockSpec(memory_space=pltpu.SMEM), pl.BlockSpec(memory_space=pltpu.VMEM)],
        out_specs=pl.BlockSpec(memory_space=pltpu.VMEM),
        compiler_params=params(SMALL_MIB),
        cost_estimate=cost(1000000, 2 * table.size + 2 * devices * count * HALF * HEAD_DIM),
        name="pick_stripes",
    )(named, table)


def lanes_of(square):
    return jnp.sum(square.T, axis=0, keepdims=True)


def columns_of(head):
    return slice(head * HEAD_DIM, (head + 1) * HEAD_DIM)


def softmax_down(scores, scale):
    weights = jnp.exp2((scores - jnp.max(scores, axis=0, keepdims=True)) * scale)
    return (weights * (1.0 / jnp.sum(weights, axis=0, keepdims=True))).astype(BF16)


def softmax_across(scores):
    weights = jnp.exp2(scores - jnp.max(scores, axis=1, keepdims=True))
    return (weights * (1.0 / jnp.sum(weights, axis=1, keepdims=True))).astype(BF16)


def self_kernel(query_ref, key_ref, value_ref, out_ref, squares_ref):
    n = pl.program_id(0)
    heads = range(query_ref.shape[1] // HEAD_DIM)
    at = [columns_of(head) for head in heads]
    scores = [dot(key_ref[:, at[h]], query_ref[:, at[h]], (1, 1)) for h in heads]
    weights = [softmax_down(scores[h], SCALE2) for h in heads]
    sums = [dot(weights[h], value_ref[:, at[h]], (0, 0)) for h in heads]
    total = jnp.zeros((NBR_LEN, HEAD_DIM), F32)
    for h in heads:
        rows = sums[h].astype(BF16)
        out_ref[:, at[h]] = rows
        wide = rows.astype(F32)
        total = total + wide * wide
    squares_ref[pl.ds(n, 1), :] = lanes_of(total)


def self_attention(query, key, value):
    rows, columns = query.shape
    count = rows // NBR_LEN
    block = pl.BlockSpec((NBR_LEN, columns), lambda n: (n, 0))
    return pl.pallas_call(
        self_kernel,
        grid=(count,),
        out_shape=(
            jax.ShapeDtypeStruct((rows, columns), BF16),
            jax.ShapeDtypeStruct((count, NBR_LEN), F32),
        ),
        in_specs=[block, block, block],
        out_specs=(block, pl.BlockSpec((count, NBR_LEN), lambda n: (0, 0))),
        compiler_params=params(SELF_MIB),
        cost_estimate=cost(8000000000, 8 * rows * columns, rows * columns),
        name="self_attention",
    )(query, key, value)


def cross_kernel(first, full_width, self_ref, got_ref, totals_ref, out_ref, squares_ref):
    n = pl.program_id(0)
    count = self_ref.shape[1] // HEAD_DIM
    heads = range(count)
    at = [columns_of(head) for head in heads]
    scale = lax.rsqrt(totals_ref[pl.ds(first + n, 1), :] / full_width + EPSILON) * SCALE2
    keys = [jnp.concatenate([got_ref[h], got_ref[count + h]], axis=0) for h in heads]
    scores = [dot(keys[h], self_ref[:, at[h]], (1, 1)) for h in heads]
    weights = [softmax_down(scores[h], scale) for h in heads]
    values = [jnp.concatenate([got_ref[2 * count + h], got_ref[3 * count + h]], axis=0) for h in heads]
    sums = [dot(weights[h], values[h], (0, 0)) for h in heads]
    total = jnp.zeros((NBR_LEN, HEAD_DIM), F32)
    for h in heads:
        crossed = sums[h].astype(BF16)
        rows = (self_ref[:, at[h]].astype(F32) + crossed.astype(F32)).astype(BF16)
        out_ref[:, at[h]] = rows
        wide = rows.astype(F32)
        total = total + wide * wide
    squares_ref[pl.ds(n, 1), :] = lanes_of(total)


def cross_attention(self_out, got, totals, first, count, full_width):
    columns = self_out.shape[1]
    rows = count * NBR_LEN
    return pl.pallas_call(
        functools.partial(cross_kernel, first, full_width),
        grid=(count,),
        out_shape=(
            jax.ShapeDtypeStruct((rows, columns), BF16),
            jax.ShapeDtypeStruct((count, NBR_LEN), F32),
        ),
        in_specs=[
            pl.BlockSpec((NBR_LEN, columns), lambda n: (first + n, 0)),
            pl.BlockSpec((got.shape[0], HALF, HEAD_DIM), lambda n: (0, first + n, 0)),
            pl.BlockSpec(totals.shape, lambda n: (0, 0)),
        ],
        out_specs=(
            pl.BlockSpec((NBR_LEN, columns), lambda n: (n, 0)),
            pl.BlockSpec((count, NBR_LEN), lambda n: (0, 0)),
        ),
        compiler_params=params(SMALL_MIB),
        cost_estimate=cost(1000000000 * count, 6 * rows * columns, rows * columns // 2),
        name="cross_attention",
    )(self_out, got, totals)


def decode_kernel(full_width, query_ref, came_ref, rest_ref, totals_ref, out_ref, prior_ref):
    u = pl.program_id(0)

    @pl.when(u == 0)
    def _():
        prior_ref[...] = came_ref[...]

    @pl.when(u > 0)
    def _():
        prior_ref[...] = rest_ref[...]

    heads = range(query_ref.shape[1] // HEAD_DIM)
    at = [columns_of(head) for head in heads]
    scale = lax.rsqrt(totals_ref[u] / full_width + EPSILON) * SCALE2
    scores = [dot(query_ref[:, at[h]], prior_ref[:, at[h]], (1, 1)) for h in heads]
    weights = [softmax_across(scores[h] * scale) for h in heads]
    for h in heads:
        out_ref[:, at[h]] = dot(weights[h], prior_ref[:, at[h]], (1, 0)).astype(BF16)


def decode(query, came, rest, totals, full_width):
    columns = query.shape[1]
    panel = NEIGHBOURS * NBR_LEN
    query_block = pl.BlockSpec((SEG_LEN, columns), lambda u: (u, 0))
    return pl.pallas_call(
        functools.partial(decode_kernel, full_width),
        grid=(SEG_DEV,),
        out_shape=jax.ShapeDtypeStruct(query.shape, BF16),
        in_specs=[
            query_block,
            pl.BlockSpec((panel, columns), lambda u: (0, 0)),
            pl.BlockSpec((panel, columns), lambda u: (jnp.maximum(u - 1, 0), 0)),
            pl.BlockSpec((SEG_DEV, 1, panel), lambda u: (0, 0, 0)),
        ],
        out_specs=query_block,
        scratch_shapes=[pltpu.VMEM((panel, columns), BF16)],
        compiler_params=params(SMALL_MIB),
        cost_estimate=cost(4000000000, 4 * query.size + 2 * (came.size + rest.size), query.size * 2),
        name="decode",
    )(query, came, rest, totals.reshape(SEG_DEV, 1, panel))


def over_heads(part):
    heads = lax.axis_size("head")
    total = part
    for step in range(1, heads):
        total = total + lax.ppermute(part, "head", [(i, (i + step) % heads) for i in range(heads)])
    return total


def from_behind(part):
    devices = lax.axis_size("span")
    return lax.ppermute(part, "span", [(i, i + 1) for i in range(devices - 1)])


def exchange(x):
    return lax.all_to_all(x, "span", split_axis=0, concat_axis=0, tiled=True)


def body(
    neighbour_query,
    neighbour_key,
    neighbour_value,
    segment_key,
    segment_value,
    decoder_query,
    sources,
):
    columns = neighbour_query.shape[1]
    full_width = columns * lax.axis_size("head")
    per_device = SEG_DEV * NEIGHBOURS
    table = exchange(pack(sources, segment_key, segment_value))
    self_out, squares = self_attention(neighbour_query, neighbour_key, neighbour_value)
    totals = over_heads(squares)
    table, totals = lax.optimization_barrier((table, totals))
    named = table[:, SEG_DEV * HALF, :per_device].astype(jnp.int32)
    got = exchange(pick(named, table))
    last = per_device - NEIGHBOURS
    panel, panel_squares = cross_attention(self_out, got, totals, last, NEIGHBOURS, full_width)
    came_squares = from_behind(panel_squares)
    came = from_behind(panel)
    rest, rest_squares = cross_attention(self_out, got, totals, 0, last, full_width)
    used = over_heads(jnp.concatenate([came_squares, rest_squares], axis=0))
    return decode(decoder_query, came, rest, used, full_width)


def solution(mesh):
    placed = (
        P("span", "head"),
        P("span", "head"),
        P("span", "head"),
        P("span", "head"),
        P("span", "head"),
        P("span", "head"),
        P("span", None),
    )
    return jax.shard_map(
        body, mesh=mesh, in_specs=placed, out_specs=P("span", "head"), check_vma=False
    )
```

```python
import functools

import jax
import jax.numpy as jnp
from jax import lax
from jax.experimental import pallas as pl
from jax.experimental.pallas import tpu as pltpu
from jax.sharding import PartitionSpec as P

HEAD_DIM = 128
SEG_LEN = 64
NBR_LEN = 128
NEIGHBOURS = 2
SEG_DEV = 4

EPSILON = 1e-06
LOG2E = 1.4426950408889634
SCALE2 = HEAD_DIM ** (-0.5) * LOG2E
HALF = SEG_LEN // 2
TAIL = 8
PACK_MIB = 60
SELF_MIB = 60
PICK_MIB = 24
SMALL_MIB = 24

F32 = jnp.float32
BF16 = jnp.bfloat16


def dot(a, b, contract):
    return lax.dot_general(a, b, ((contract[:1], contract[1:]), ((), ())), preferred_element_type=F32)


def cost(flops, moved, exps=0):
    return pl.CostEstimate(flops=flops, bytes_accessed=moved, transcendentals=exps)


def params(mib):
    return pltpu.CompilerParams(vmem_limit_bytes=mib * 1024 * 1024)


def in_hbm(x):
    return pltpu.with_memory_space_constraint(x, pltpu.HBM)


def pack_kernel(sources_ref, key_ref, value_ref, out_ref, rows_ref, packed_ref, in_sems, out_sems):
    heads = key_ref.shape[1] // HEAD_DIM

    def into(kv, seg):
        at = pl.ds(seg * SEG_LEN, SEG_LEN)
        ref = (key_ref, value_ref)[kv]
        return pltpu.make_async_copy(ref.at[at, :], rows_ref.at[kv, at, :], in_sems.at[kv, seg])

    def out_of(seg):
        at = pl.ds(seg * HALF, HALF + TAIL if seg == SEG_DEV - 1 else HALF)
        return pltpu.make_async_copy(packed_ref.at[:, at, :], out_ref.at[:, at, :], out_sems.at[seg])

    for seg in range(SEG_DEV):
        for kv in range(2):
            into(kv, seg).start()
    lane = lax.broadcasted_iota(jnp.int32, (TAIL, HEAD_DIM), 1)
    tail = jnp.zeros((TAIL, HEAD_DIM), F32)
    for i in range(SEG_DEV * NEIGHBOURS):
        named = sources_ref[i % NEIGHBOURS, i // NEIGHBOURS].astype(F32)
        tail = jnp.where(lane == i, named, tail)
    tail = tail.astype(BF16)
    for stripe in range(4 * heads):
        packed_ref[stripe, SEG_DEV * HALF:SEG_DEV * HALF + TAIL, :] = tail
    for seg in range(SEG_DEV):
        for kv in range(2):
            into(kv, seg).wait()
            for half in range(2):
                row = seg * SEG_LEN + half * HALF
                for head in range(heads):
                    packed_ref[(kv * 2 + half) * heads + head, seg * HALF:(seg + 1) * HALF, :] = rows_ref[
                        kv, row:row + HALF, head * HEAD_DIM:(head + 1) * HEAD_DIM
                    ]
        out_of(seg).start()
    for seg in range(SEG_DEV):
        out_of(seg).wait()


def pack(sources, segment_key, segment_value):
    rows, columns = segment_key.shape
    shape = (4 * columns // HEAD_DIM, SEG_DEV * HALF + TAIL, HEAD_DIM)
    hbm = pl.BlockSpec(memory_space=pl.ANY)
    return pl.pallas_call(
        pack_kernel,
        out_shape=jax.ShapeDtypeStruct(shape, BF16),
        in_specs=[pl.BlockSpec(memory_space=pltpu.SMEM), hbm, hbm],
        out_specs=hbm,
        scratch_shapes=[
            pltpu.VMEM((2, rows, columns), BF16),
            pltpu.VMEM(shape, BF16),
            pltpu.SemaphoreType.DMA((2, SEG_DEV)),
            pltpu.SemaphoreType.DMA((SEG_DEV,)),
        ],
        compiler_params=params(PACK_MIB),
        cost_estimate=cost(1000000, 2 * 2 * segment_key.size * 2),
        name="pack_stripes",
    )(sources.T, segment_key, segment_value)


def pick_kernel(named_ref, table_ref, out_ref):
    here = out_ref.shape[0]
    devices = table_ref.shape[0]
    first = pl.program_id(0) * here
    count = SEG_DEV * NEIGHBOURS

    def one(step, carry):
        device = first + step
        behind = lax.rem(device + devices - 1, devices)
        for i in range(count):
            if i < NEIGHBOURS:
                named = named_ref[behind, count - NEIGHBOURS + i]
            else:
                named = named_ref[device, i - NEIGHBOURS]
            owner = lax.shift_right_logical(named, 2)
            within = lax.bitwise_and(named, SEG_DEV - 1)
            start = pl.multiple_of(within * HALF, HALF)
            out_ref[step, i * HALF:(i + 1) * HALF, :] = table_ref[owner, pl.ds(start, HALF), :]
        return carry

    lax.fori_loop(0, here, one, 0, unroll=2)


def pick(named, table):
    devices = table.shape[0]
    count = SEG_DEV * NEIGHBOURS
    steps = 4
    return pl.pallas_call(
        pick_kernel,
        grid=(steps,),
        out_shape=jax.ShapeDtypeStruct((devices, count * HALF, HEAD_DIM), BF16),
        in_specs=[
            pl.BlockSpec(memory_space=pltpu.SMEM),
            pl.BlockSpec(table.shape, lambda i: (0, 0, 0)),
        ],
        out_specs=pl.BlockSpec((devices // steps, count * HALF, HEAD_DIM), lambda i: (i, 0, 0)),
        compiler_params=params(PICK_MIB),
        cost_estimate=cost(1000000, 2 * table.size + 2 * devices * count * HALF * HEAD_DIM),
        name="pick_stripes",
    )(named, table)


def lanes_of(square):
    return jnp.sum(square.T, axis=0, keepdims=True)


def columns_of(head):
    return slice(head * HEAD_DIM, (head + 1) * HEAD_DIM)


def softmax_down(scores, scale):
    weights = jnp.exp2((scores - jnp.max(scores, axis=0, keepdims=True)) * scale)
    return (weights * (1.0 / jnp.sum(weights, axis=0, keepdims=True))).astype(BF16)


def softmax_across(scores):
    weights = jnp.exp2(scores - jnp.max(scores, axis=1, keepdims=True))
    return (weights * (1.0 / jnp.sum(weights, axis=1, keepdims=True))).astype(BF16)


def self_kernel(query_ref, key_ref, value_ref, out_ref, squares_ref):
    n = pl.program_id(0)
    heads = range(query_ref.shape[1] // HEAD_DIM)
    at = [columns_of(head) for head in heads]
    scores = [dot(key_ref[:, at[h]], query_ref[:, at[h]], (1, 1)) for h in heads]
    weights = [softmax_down(scores[h], SCALE2) for h in heads]
    sums = [dot(weights[h], value_ref[:, at[h]], (0, 0)) for h in heads]
    total = jnp.zeros((NBR_LEN, HEAD_DIM), F32)
    for h in heads:
        rows = sums[h].astype(BF16)
        out_ref[:, at[h]] = rows
        wide = rows.astype(F32)
        total = total + wide * wide
    squares_ref[pl.ds(n, 1), :] = lanes_of(total)


def self_attention(query, key, value, first, count):
    columns = query.shape[1]
    rows = count * NBR_LEN
    block = pl.BlockSpec((NBR_LEN, columns), lambda n: (first + n, 0))
    return pl.pallas_call(
        self_kernel,
        grid=(count,),
        out_shape=(
            jax.ShapeDtypeStruct((rows, columns), BF16),
            jax.ShapeDtypeStruct((count, NBR_LEN), F32),
        ),
        in_specs=[block, block, block],
        out_specs=(
            pl.BlockSpec((NBR_LEN, columns), lambda n: (n, 0)),
            pl.BlockSpec((count, NBR_LEN), lambda n: (0, 0)),
        ),
        compiler_params=params(SELF_MIB),
        cost_estimate=cost(1000000000 * count, 8 * rows * columns, rows * columns),
        name="self_attention",
    )(query, key, value)


def cross_kernel(first, full_width, self_ref, got_ref, totals_ref, out_ref, squares_ref):
    n = pl.program_id(0)
    count = self_ref.shape[1] // HEAD_DIM
    heads = range(count)
    at = [columns_of(head) for head in heads]
    scale = lax.rsqrt(totals_ref[pl.ds(first + n, 1), :] / full_width + EPSILON) * SCALE2
    keys = [jnp.concatenate([got_ref[h], got_ref[count + h]], axis=0) for h in heads]
    scores = [dot(keys[h], self_ref[:, at[h]], (1, 1)) for h in heads]
    weights = [softmax_down(scores[h], scale) for h in heads]
    values = [jnp.concatenate([got_ref[2 * count + h], got_ref[3 * count + h]], axis=0) for h in heads]
    sums = [dot(weights[h], values[h], (0, 0)) for h in heads]
    total = jnp.zeros((NBR_LEN, HEAD_DIM), F32)
    for h in heads:
        crossed = sums[h].astype(BF16)
        rows = (self_ref[:, at[h]].astype(F32) + crossed.astype(F32)).astype(BF16)
        out_ref[:, at[h]] = rows
        wide = rows.astype(F32)
        total = total + wide * wide
    squares_ref[pl.ds(n, 1), :] = lanes_of(total)


def cross_attention(self_rows, got, totals, first, full_width):
    rows, columns = self_rows.shape
    count = rows // NBR_LEN
    block = pl.BlockSpec((NBR_LEN, columns), lambda n: (n, 0))
    return pl.pallas_call(
        functools.partial(cross_kernel, first, full_width),
        grid=(count,),
        out_shape=(
            pltpu.HBM((rows, columns), BF16),
            jax.ShapeDtypeStruct((count, NBR_LEN), F32),
        ),
        in_specs=[
            block,
            pl.BlockSpec((got.shape[0], HALF, HEAD_DIM), lambda n: (0, first + n, 0)),
            pl.BlockSpec(totals.shape, lambda n: (0, 0)),
        ],
        out_specs=(block, pl.BlockSpec((count, NBR_LEN), lambda n: (0, 0))),
        compiler_params=params(SMALL_MIB),
        cost_estimate=cost(1000000000 * count, 6 * rows * columns, rows * columns // 2),
        name="cross_attention",
    )(in_hbm(self_rows), got, totals)


def decode_kernel(full_width, place_ref, query_ref, came_ref, rest_ref, totals_ref, out_ref, prior_ref):
    u = pl.program_id(0)

    @pl.when(u == 0)
    def _():
        prior_ref[...] = came_ref[...]

    @pl.when(u > 0)
    def _():
        prior_ref[...] = rest_ref[...]

    empty = (u == 0) & (place_ref[0] == 0)
    heads = range(query_ref.shape[1] // HEAD_DIM)
    at = [columns_of(head) for head in heads]
    scale = lax.rsqrt(totals_ref[u] / full_width + EPSILON) * SCALE2
    scores = [dot(query_ref[:, at[h]], prior_ref[:, at[h]], (1, 1)) for h in heads]
    weights = [softmax_across(scores[h] * scale) for h in heads]
    for h in heads:
        rows = dot(weights[h], prior_ref[:, at[h]], (1, 0))
        out_ref[:, at[h]] = jnp.where(empty, 0.0, rows).astype(BF16)


def decode(place, query, came, rest, totals, full_width):
    columns = query.shape[1]
    panel = NEIGHBOURS * NBR_LEN
    query_block = pl.BlockSpec((SEG_LEN, columns), lambda u: (u, 0))
    return pl.pallas_call(
        functools.partial(decode_kernel, full_width),
        grid=(SEG_DEV,),
        out_shape=jax.ShapeDtypeStruct(query.shape, BF16),
        in_specs=[
            pl.BlockSpec(memory_space=pltpu.SMEM),
            query_block,
            pl.BlockSpec((panel, columns), lambda u: (0, 0)),
            pl.BlockSpec((panel, columns), lambda u: (jnp.maximum(u - 1, 0), 0)),
            pl.BlockSpec((SEG_DEV, 1, panel), lambda u: (0, 0, 0)),
        ],
        out_specs=query_block,
        scratch_shapes=[pltpu.VMEM((panel, columns), BF16)],
        compiler_params=params(SMALL_MIB),
        cost_estimate=cost(4000000000, 4 * query.size + 2 * (came.size + rest.size), query.size * 2),
        name="decode",
    )(place, in_hbm(query), in_hbm(came), in_hbm(rest), totals.reshape(SEG_DEV, 1, panel))


def over_heads(part):
    heads = lax.axis_size("head")
    total = part
    for step in range(1, heads):
        total = total + lax.ppermute(part, "head", [(i, (i + step) % heads) for i in range(heads)])
    return total


def from_behind(part):
    devices = lax.axis_size("span")
    return lax.ppermute(part, "span", [(i, i + 1) for i in range(devices - 1)])


def exchange(x):
    return lax.all_to_all(x, "span", split_axis=0, concat_axis=0, tiled=True)


def body(
    neighbour_query,
    neighbour_key,
    neighbour_value,
    segment_key,
    segment_value,
    decoder_query,
    sources,
):
    columns = neighbour_query.shape[1]
    full_width = columns * lax.axis_size("head")
    per_device = SEG_DEV * NEIGHBOURS
    last = per_device - NEIGHBOURS
    triple = (neighbour_query, neighbour_key, neighbour_value)
    table = exchange(pack(sources, segment_key, segment_value))
    panel, panel_squares = self_attention(*triple, last, NEIGHBOURS)
    came = from_behind(panel)
    rest, rest_squares = self_attention(*triple, 0, last)
    table, came, panel_squares, rest_squares = lax.optimization_barrier((table, came, panel_squares, rest_squares))
    named = table[:, SEG_DEV * HALF, :per_device].astype(jnp.int32)
    got = exchange(pick(named, table))
    totals = over_heads(jnp.concatenate([from_behind(panel_squares), rest_squares], axis=0))
    came, came_squares = cross_attention(came, got, totals, 0, full_width)
    rest, rest_squares = cross_attention(rest, got, totals, NEIGHBOURS, full_width)
    used = over_heads(jnp.concatenate([came_squares, rest_squares], axis=0))
    place = lax.axis_index("span").astype(jnp.int32).reshape(1)
    return decode(place, decoder_query, came, rest, used, full_width)


def solution(mesh):
    placed = (
        P("span", "head"),
        P("span", "head"),
        P("span", "head"),
        P("span", "head"),
        P("span", "head"),
        P("span", "head"),
        P("span", None),
    )
    return jax.shard_map(
        body, mesh=mesh, in_specs=placed, out_specs=P("span", "head"), check_vma=False
    )
```

```python
import functools

import jax
import jax.numpy as jnp
from jax import lax
from jax.experimental import pallas as pl
from jax.experimental.pallas import tpu as pltpu
from jax.sharding import PartitionSpec as P


HEAD_DIM = 128
SEG_LEN = 64
NBR_LEN = 128
NEIGHBOURS = 2
SEG_DEV = 4

EPSILON = 1e-06
LOG2E = 1.4426950408889634
SCALE2 = HEAD_DIM ** (-0.5) * LOG2E
HALF = SEG_LEN // 2
TAIL = 8
PACK_MIB = 60
SELF_MIB = 24
PICK_MIB = 24
SMALL_MIB = 24

F32 = jnp.float32
BF16 = jnp.bfloat16


def dot(a, b, contract):
    return lax.dot_general(a, b, ((contract[:1], contract[1:]), ((), ())), preferred_element_type=F32)


def cost(flops, moved, exps=0):
    return pl.CostEstimate(flops=flops, bytes_accessed=moved, transcendentals=exps)


def params(mib):
    return pltpu.CompilerParams(vmem_limit_bytes=mib * 1024 * 1024)


def in_hbm(x):
    return pltpu.with_memory_space_constraint(x, pltpu.HBM)


def pack_kernel(sources_ref, key_ref, value_ref, out_ref, rows_ref, packed_ref, in_sems, out_sems):
    heads = key_ref.shape[1] // HEAD_DIM

    def into(kv, seg):
        at = pl.ds(seg * SEG_LEN, SEG_LEN)
        ref = (key_ref, value_ref)[kv]
        return pltpu.make_async_copy(ref.at[at, :], rows_ref.at[kv, at, :], in_sems.at[kv, seg])

    def out_of(seg):
        at = pl.ds(seg * HALF, HALF + TAIL if seg == SEG_DEV - 1 else HALF)
        return pltpu.make_async_copy(packed_ref.at[:, at, :], out_ref.at[:, at, :], out_sems.at[seg])

    for seg in range(SEG_DEV):
        for kv in range(2):
            into(kv, seg).start()
    lane = lax.broadcasted_iota(jnp.int32, (TAIL, HEAD_DIM), 1)
    tail = jnp.zeros((TAIL, HEAD_DIM), F32)
    for i in range(SEG_DEV * NEIGHBOURS):
        named = sources_ref[i % NEIGHBOURS, i // NEIGHBOURS].astype(F32)
        tail = jnp.where(lane == i, named, tail)
    tail = tail.astype(BF16)
    for stripe in range(4 * heads):
        packed_ref[stripe, SEG_DEV * HALF:SEG_DEV * HALF + TAIL, :] = tail
    for seg in range(SEG_DEV):
        for kv in range(2):
            into(kv, seg).wait()
            for half in range(2):
                row = seg * SEG_LEN + half * HALF
                for head in range(heads):
                    packed_ref[(kv * 2 + half) * heads + head, seg * HALF:(seg + 1) * HALF, :] = rows_ref[
                        kv, row:row + HALF, head * HEAD_DIM:(head + 1) * HEAD_DIM
                    ]
        out_of(seg).start()
    for seg in range(SEG_DEV):
        out_of(seg).wait()


def pack(sources, segment_key, segment_value):
    rows, columns = segment_key.shape
    shape = (4 * columns // HEAD_DIM, SEG_DEV * HALF + TAIL, HEAD_DIM)
    hbm = pl.BlockSpec(memory_space=pl.ANY)
    return pl.pallas_call(
        pack_kernel,
        out_shape=jax.ShapeDtypeStruct(shape, BF16),
        in_specs=[pl.BlockSpec(memory_space=pltpu.SMEM), hbm, hbm],
        out_specs=hbm,
        scratch_shapes=[
            pltpu.VMEM((2, rows, columns), BF16),
            pltpu.VMEM(shape, BF16),
            pltpu.SemaphoreType.DMA((2, SEG_DEV)),
            pltpu.SemaphoreType.DMA((SEG_DEV,)),
        ],
        compiler_params=params(PACK_MIB),
        cost_estimate=cost(1000000, 2 * 2 * segment_key.size * 2),
        name="pack_stripes",
    )(sources.T, segment_key, segment_value)


def pick_kernel(named_ref, table_ref, out_ref):
    here = out_ref.shape[0]
    devices = table_ref.shape[0]
    first = pl.program_id(0) * here
    count = SEG_DEV * NEIGHBOURS

    def one(step, carry):
        device = first + step
        behind = lax.rem(device + devices - 1, devices)
        for i in range(count):
            if i < NEIGHBOURS:
                named = named_ref[behind, count - NEIGHBOURS + i]
            else:
                named = named_ref[device, i - NEIGHBOURS]
            owner = lax.shift_right_logical(named, 2)
            within = lax.bitwise_and(named, SEG_DEV - 1)
            start = pl.multiple_of(within * HALF, HALF)
            out_ref[step, i * HALF:(i + 1) * HALF, :] = table_ref[owner, pl.ds(start, HALF), :]
        return carry

    lax.fori_loop(0, here, one, 0, unroll=2)


def pick(named, table):
    devices = table.shape[0]
    count = SEG_DEV * NEIGHBOURS
    steps = 4
    return pl.pallas_call(
        pick_kernel,
        grid=(steps,),
        out_shape=jax.ShapeDtypeStruct((devices, count * HALF, HEAD_DIM), BF16),
        in_specs=[
            pl.BlockSpec(memory_space=pltpu.SMEM),
            pl.BlockSpec(table.shape, lambda i: (0, 0, 0)),
        ],
        out_specs=pl.BlockSpec((devices // steps, count * HALF, HEAD_DIM), lambda i: (i, 0, 0)),
        compiler_params=params(PICK_MIB),
        cost_estimate=cost(1000000, 2 * table.size + 2 * devices * count * HALF * HEAD_DIM),
        name="pick_stripes",
    )(named, table)


def lanes_of(square):
    return jnp.sum(square.T, axis=0, keepdims=True)


def columns_of(head):
    return slice(head * HEAD_DIM, (head + 1) * HEAD_DIM)


def softmax_down(scores, scale):
    weights = jnp.exp2((scores - jnp.max(scores, axis=0, keepdims=True)) * scale)
    return (weights * (1.0 / jnp.sum(weights, axis=0, keepdims=True))).astype(BF16)


def softmax_across(scores):
    weights = jnp.exp2(scores - jnp.max(scores, axis=1, keepdims=True))
    return (weights * (1.0 / jnp.sum(weights, axis=1, keepdims=True))).astype(BF16)


def self_kernel(query_ref, key_ref, value_ref, out_ref, squares_ref):
    n = pl.program_id(0)
    heads = range(query_ref.shape[1] // HEAD_DIM)
    at = [columns_of(head) for head in heads]
    scores = [dot(key_ref[:, at[h]], query_ref[:, at[h]], (1, 1)) for h in heads]
    weights = [softmax_down(scores[h], SCALE2) for h in heads]
    sums = [dot(weights[h], value_ref[:, at[h]], (0, 0)) for h in heads]
    total = jnp.zeros((NBR_LEN, HEAD_DIM), F32)
    for h in heads:
        rows = sums[h].astype(BF16)
        out_ref[:, at[h]] = rows
        wide = rows.astype(F32)
        total = total + wide * wide
    squares_ref[pl.ds(n, 1), :] = lanes_of(total)


def self_attention(query, key, value, first, count, held=jax.ShapeDtypeStruct):
    columns = query.shape[1]
    rows = count * NBR_LEN
    block = pl.BlockSpec((NBR_LEN, columns), lambda n: (first + n, 0))
    return pl.pallas_call(
        self_kernel,
        grid=(count,),
        out_shape=(
            held((rows, columns), BF16),
            jax.ShapeDtypeStruct((count, NBR_LEN), F32),
        ),
        in_specs=[block, block, block],
        out_specs=(
            pl.BlockSpec((NBR_LEN, columns), lambda n: (n, 0)),
            pl.BlockSpec((count, NBR_LEN), lambda n: (0, 0)),
        ),
        compiler_params=params(SELF_MIB),
        cost_estimate=cost(1000000000 * count, 8 * rows * columns, rows * columns),
        name="self_attention",
    )(in_hbm(query), in_hbm(key), in_hbm(value))


def squares_kernel(rows_ref, own_ref, squares_ref):
    for n in range(NEIGHBOURS):
        total = jnp.zeros((NBR_LEN, HEAD_DIM), F32)
        for head in range(rows_ref.shape[1] // HEAD_DIM):
            wide = rows_ref[n * NBR_LEN:(n + 1) * NBR_LEN, columns_of(head)].astype(F32)
            total = total + wide * wide
        squares_ref[n:n + 1, :] = lanes_of(total)
    squares_ref[NEIGHBOURS:, :] = own_ref[...]


def squares_above(rows, own):
    vmem = pl.BlockSpec(memory_space=pltpu.VMEM)
    return pl.pallas_call(
        squares_kernel,
        out_shape=jax.ShapeDtypeStruct((NEIGHBOURS + own.shape[0], NBR_LEN), F32),
        in_specs=[vmem, vmem],
        out_specs=vmem,
        compiler_params=params(SMALL_MIB),
        cost_estimate=cost(1000000000, 2 * rows.size),
        name="row_squares",
    )(rows, own)


def summed(refs, at):
    return functools.reduce(lambda a, b: a + b, [ref[at, :] for ref in refs])


def cross_kernel(full_width, came_ref, rest_ref, got_ref, *refs):
    parts, (out_ref, squares_ref, self_ref) = refs[:-3], refs[-3:]
    n = pl.program_id(0)

    @pl.when(n < NEIGHBOURS)
    def _():
        self_ref[...] = came_ref[...]

    @pl.when(n >= NEIGHBOURS)
    def _():
        self_ref[...] = rest_ref[...]

    count = self_ref.shape[1] // HEAD_DIM
    heads = range(count)
    at = [columns_of(head) for head in heads]
    scale = lax.rsqrt(summed(parts, pl.ds(n, 1)) / full_width + EPSILON) * SCALE2
    keys = [jnp.concatenate([got_ref[h], got_ref[count + h]], axis=0) for h in heads]
    scores = [dot(keys[h], self_ref[:, at[h]], (1, 1)) for h in heads]
    weights = [softmax_down(scores[h], scale) for h in heads]
    values = [jnp.concatenate([got_ref[2 * count + h], got_ref[3 * count + h]], axis=0) for h in heads]
    sums = [dot(weights[h], values[h], (0, 0)) for h in heads]
    total = jnp.zeros((NBR_LEN, HEAD_DIM), F32)
    for h in heads:
        crossed = sums[h].astype(BF16)
        rows = (self_ref[:, at[h]].astype(F32) + crossed.astype(F32)).astype(BF16)
        out_ref[:, at[h]] = rows
        wide = rows.astype(F32)
        total = total + wide * wide
    squares_ref[pl.ds(n, 1), :] = lanes_of(total)


def cross_attention(came, rest, got, parts, full_width):
    columns = came.shape[1]
    count = SEG_DEV * NEIGHBOURS
    rows = count * NBR_LEN
    sums = pl.BlockSpec((count, NBR_LEN), lambda n: (0, 0))
    return pl.pallas_call(
        functools.partial(cross_kernel, full_width),
        grid=(count,),
        out_shape=(
            jax.ShapeDtypeStruct((rows, columns), BF16),
            jax.ShapeDtypeStruct((count, NBR_LEN), F32),
        ),
        in_specs=[
            pl.BlockSpec((NBR_LEN, columns), lambda n: (jnp.minimum(n, NEIGHBOURS - 1), 0)),
            pl.BlockSpec((NBR_LEN, columns), lambda n: (jnp.maximum(n - NEIGHBOURS, 0), 0)),
            pl.BlockSpec((got.shape[0], HALF, HEAD_DIM), lambda n: (0, n, 0)),
        ]
        + [sums] * len(parts),
        out_specs=(pl.BlockSpec((NBR_LEN, columns), lambda n: (n, 0)), sums),
        scratch_shapes=[pltpu.VMEM((NBR_LEN, columns), BF16)],
        compiler_params=params(SMALL_MIB),
        cost_estimate=cost(1000000000 * count, 6 * rows * columns, rows * columns // 2),
        name="cross_attention",
    )(came, rest, got, *parts)


def decode_kernel(full_width, place_ref, query_ref, prior_ref, *refs):
    parts, out_ref = refs[:-1], refs[-1]
    u = pl.program_id(0)
    empty = (u == 0) & (place_ref[0] == 0)
    heads = range(query_ref.shape[1] // HEAD_DIM)
    at = [columns_of(head) for head in heads]
    totals = [summed(parts, pl.ds(u * NEIGHBOURS + n, 1)) for n in range(NEIGHBOURS)]
    scale = lax.rsqrt(jnp.concatenate(totals, axis=1) / full_width + EPSILON) * SCALE2
    scores = [dot(query_ref[:, at[h]], prior_ref[:, at[h]], (1, 1)) for h in heads]
    weights = [softmax_across(scores[h] * scale) for h in heads]
    for h in heads:
        rows = dot(weights[h], prior_ref[:, at[h]], (1, 0))
        out_ref[:, at[h]] = jnp.where(empty, 0.0, rows).astype(BF16)


def decode(place, query, prior, parts, full_width):
    columns = query.shape[1]
    panel = NEIGHBOURS * NBR_LEN
    query_block = pl.BlockSpec((SEG_LEN, columns), lambda u: (u, 0))
    sums = pl.BlockSpec(parts[0].shape, lambda u: (0, 0))
    return pl.pallas_call(
        functools.partial(decode_kernel, full_width),
        grid=(SEG_DEV,),
        out_shape=jax.ShapeDtypeStruct(query.shape, BF16),
        in_specs=[
            pl.BlockSpec(memory_space=pltpu.SMEM),
            query_block,
            pl.BlockSpec((panel, columns), lambda u: (u, 0)),
        ]
        + [sums] * len(parts),
        out_specs=query_block,
        compiler_params=params(SMALL_MIB),
        cost_estimate=cost(4000000000, 4 * query.size + 2 * prior.size, query.size * 2),
        name="decode",
    )(place, query, prior, *parts)


def over_heads(part):
    heads = lax.axis_size("head")
    return [part] + [
        lax.ppermute(part, "head", [(i, (i + step) % heads) for i in range(heads)])
        for step in range(1, heads)
    ]


def from_behind(part):
    devices = lax.axis_size("span")
    return lax.ppermute(part, "span", [(i, i + 1) for i in range(devices - 1)])


def exchange(x):
    return lax.all_to_all(x, "span", split_axis=0, concat_axis=0, tiled=True)


def body(
    neighbour_query,
    neighbour_key,
    neighbour_value,
    segment_key,
    segment_value,
    decoder_query,
    sources,
):
    columns = neighbour_query.shape[1]
    full_width = columns * lax.axis_size("head")
    per_device = SEG_DEV * NEIGHBOURS
    last = per_device - NEIGHBOURS
    place = lax.axis_index("span").astype(jnp.int32).reshape(1)
    sources, place = lax.optimization_barrier((sources, place))
    triple = (neighbour_query, neighbour_key, neighbour_value)
    table = exchange(pack(sources, segment_key, segment_value))
    panel, _ = self_attention(*triple, last, NEIGHBOURS, pltpu.HBM)
    came = from_behind(panel)
    rest, rest_squares = self_attention(*triple, 0, last)
    table, rest_squares = lax.optimization_barrier((table, rest_squares))
    named = table[:, SEG_DEV * HALF, :per_device].astype(jnp.int32)
    got = exchange(pick(named, table))
    parts = over_heads(squares_above(came, rest_squares))
    encoded, squares = cross_attention(came, rest, got, parts, full_width)
    return decode(place, decoder_query, encoded, over_heads(squares), full_width)


def solution(mesh):
    placed = (
        P("span", "head"),
        P("span", "head"),
        P("span", "head"),
        P("span", "head"),
        P("span", "head"),
        P("span", "head"),
        P("span", None),
    )
    return jax.shard_map(
        body, mesh=mesh, in_specs=placed, out_specs=P("span", "head"), check_vma=False
    )
```

```python
import functools

import jax
import jax.numpy as jnp
from jax import lax
from jax.experimental import pallas as pl
from jax.experimental.pallas import tpu as pltpu
from jax.sharding import PartitionSpec as P


HEAD_DIM = 128
SEG_LEN = 64
NBR_LEN = 128
NEIGHBOURS = 2
SEG_DEV = 4

EPSILON = 1e-06
LOG2E = 1.4426950408889634
SCALE2 = HEAD_DIM ** (-0.5) * LOG2E
HALF = SEG_LEN // 2
TAIL = 8
PACK_MIB = 60
SELF_MIB = 24
PICK_MIB = 24
SMALL_MIB = 24

F32 = jnp.float32
BF16 = jnp.bfloat16


def dot(a, b, contract):
    return lax.dot_general(a, b, ((contract[:1], contract[1:]), ((), ())), preferred_element_type=F32)


def cost(flops, moved, exps=0):
    return pl.CostEstimate(flops=flops, bytes_accessed=moved, transcendentals=exps)


def params(mib):
    return pltpu.CompilerParams(vmem_limit_bytes=mib * 1024 * 1024)


def in_hbm(x):
    return pltpu.with_memory_space_constraint(x, pltpu.HBM)


def pack_kernel(sources_ref, key_ref, value_ref, out_ref, rows_ref, packed_ref, in_sems, out_sems):
    heads = key_ref.shape[1] // HEAD_DIM

    def into(kv, seg):
        at = pl.ds(seg * SEG_LEN, SEG_LEN)
        ref = (key_ref, value_ref)[kv]
        return pltpu.make_async_copy(ref.at[at, :], rows_ref.at[kv, at, :], in_sems.at[kv, seg])

    def out_of(seg):
        at = pl.ds(seg * HALF, HALF + TAIL if seg == SEG_DEV - 1 else HALF)
        return pltpu.make_async_copy(packed_ref.at[:, at, :], out_ref.at[:, at, :], out_sems.at[seg])

    for seg in range(SEG_DEV):
        for kv in range(2):
            into(kv, seg).start()
    lane = lax.broadcasted_iota(jnp.int32, (TAIL, HEAD_DIM), 1)
    tail = jnp.zeros((TAIL, HEAD_DIM), F32)
    for i in range(SEG_DEV * NEIGHBOURS):
        named = sources_ref[i % NEIGHBOURS, i // NEIGHBOURS].astype(F32)
        tail = jnp.where(lane == i, named, tail)
    tail = tail.astype(BF16)
    for stripe in range(4 * heads):
        packed_ref[stripe, SEG_DEV * HALF:SEG_DEV * HALF + TAIL, :] = tail
    for seg in range(SEG_DEV):
        for kv in range(2):
            into(kv, seg).wait()
            for half in range(2):
                row = seg * SEG_LEN + half * HALF
                for head in range(heads):
                    packed_ref[(kv * 2 + half) * heads + head, seg * HALF:(seg + 1) * HALF, :] = rows_ref[
                        kv, row:row + HALF, head * HEAD_DIM:(head + 1) * HEAD_DIM
                    ]
        out_of(seg).start()
    for seg in range(SEG_DEV):
        out_of(seg).wait()


def pack(sources, segment_key, segment_value):
    rows, columns = segment_key.shape
    shape = (4 * columns // HEAD_DIM, SEG_DEV * HALF + TAIL, HEAD_DIM)
    hbm = pl.BlockSpec(memory_space=pl.ANY)
    return pl.pallas_call(
        pack_kernel,
        out_shape=jax.ShapeDtypeStruct(shape, BF16),
        in_specs=[pl.BlockSpec(memory_space=pltpu.SMEM), hbm, hbm],
        out_specs=hbm,
        scratch_shapes=[
            pltpu.VMEM((2, rows, columns), BF16),
            pltpu.VMEM(shape, BF16),
            pltpu.SemaphoreType.DMA((2, SEG_DEV)),
            pltpu.SemaphoreType.DMA((SEG_DEV,)),
        ],
        compiler_params=params(PACK_MIB),
        cost_estimate=cost(1000000, 2 * 2 * segment_key.size * 2),
        name="pack_stripes",
    )(sources.T, segment_key, segment_value)


def pick_kernel(named_ref, table_ref, out_ref, picked_ref, sems):
    devices = table_ref.shape[0]
    groups = sems.shape[0]
    here = devices // groups
    count = SEG_DEV * NEIGHBOURS

    def out_of(group):
        at = pl.ds(group * here, here)
        return pltpu.make_async_copy(picked_ref.at[at], out_ref.at[at], sems.at[group])

    def one(group, carry):
        for step in range(here):
            device = group * here + step
            behind = lax.rem(device + devices - 1, devices)
            for i in range(count):
                if i < NEIGHBOURS:
                    named = named_ref[behind, count - NEIGHBOURS + i]
                else:
                    named = named_ref[device, i - NEIGHBOURS]
                owner = lax.shift_right_logical(named, 2)
                within = lax.bitwise_and(named, SEG_DEV - 1)
                start = pl.multiple_of(within * HALF, HALF)
                picked_ref[device, i * HALF:(i + 1) * HALF, :] = table_ref[owner, pl.ds(start, HALF), :]
        out_of(group).start()
        return carry

    lax.fori_loop(0, groups, one, 0)
    for group in range(groups):
        out_of(group).wait()


def pick(named, table):
    devices = table.shape[0]
    shape = (devices, SEG_DEV * NEIGHBOURS * HALF, HEAD_DIM)
    groups = 8
    return pl.pallas_call(
        pick_kernel,
        out_shape=jax.ShapeDtypeStruct(shape, BF16),
        in_specs=[pl.BlockSpec(memory_space=pltpu.SMEM), pl.BlockSpec(memory_space=pltpu.VMEM)],
        out_specs=pl.BlockSpec(memory_space=pl.ANY),
        scratch_shapes=[pltpu.VMEM(shape, BF16), pltpu.SemaphoreType.DMA((groups,))],
        compiler_params=params(PICK_MIB),
        cost_estimate=cost(1000000, 2 * table.size + 2 * devices * shape[1] * HEAD_DIM),
        name="pick_stripes",
    )(named, table)


def lanes_of(square):
    return jnp.sum(square.T, axis=0, keepdims=True)


def columns_of(head):
    return slice(head * HEAD_DIM, (head + 1) * HEAD_DIM)


def softmax_down(scores, scale):
    weights = jnp.exp2((scores - jnp.max(scores, axis=0, keepdims=True)) * scale)
    return (weights * (1.0 / jnp.sum(weights, axis=0, keepdims=True))).astype(BF16)


def softmax_across(scores):
    weights = jnp.exp2(scores - jnp.max(scores, axis=1, keepdims=True))
    return (weights * (1.0 / jnp.sum(weights, axis=1, keepdims=True))).astype(BF16)


def self_kernel(query_ref, key_ref, value_ref, rest_ref, panel_ref, squares_ref, held_ref):
    n = pl.program_id(0)
    last = pl.num_programs(0) - NEIGHBOURS
    heads = range(query_ref.shape[1] // HEAD_DIM)
    at = [columns_of(head) for head in heads]
    scores = [dot(key_ref[:, at[h]], query_ref[:, at[h]], (1, 1)) for h in heads]
    weights = [softmax_down(scores[h], SCALE2) for h in heads]
    sums = [dot(weights[h], value_ref[:, at[h]], (0, 0)) for h in heads]
    total = jnp.zeros((NBR_LEN, HEAD_DIM), F32)
    for h in heads:
        rows = sums[h].astype(BF16)
        held_ref[:, at[h]] = rows
        wide = rows.astype(F32)
        total = total + wide * wide

    @pl.when(n < last)
    def _():
        rest_ref[...] = held_ref[...]
        squares_ref[pl.ds(n, 1), :] = lanes_of(total)

    @pl.when(n >= last)
    def _():
        panel_ref[...] = held_ref[...]


def self_attention(query, key, value):
    columns = query.shape[1]
    count = query.shape[0] // NBR_LEN
    last = count - NEIGHBOURS
    block = pl.BlockSpec((NBR_LEN, columns), lambda n: (n, 0))
    return pl.pallas_call(
        self_kernel,
        grid=(count,),
        out_shape=(
            pltpu.HBM((last * NBR_LEN, columns), BF16),
            pltpu.HBM((NEIGHBOURS * NBR_LEN, columns), BF16),
            jax.ShapeDtypeStruct((last, NBR_LEN), F32),
        ),
        in_specs=[block, block, block],
        out_specs=(
            pl.BlockSpec((NBR_LEN, columns), lambda n: (jnp.minimum(n, last - 1), 0)),
            pl.BlockSpec((NBR_LEN, columns), lambda n: (jnp.maximum(n - last, 0), 0)),
            pl.BlockSpec((last, NBR_LEN), lambda n: (0, 0)),
        ),
        scratch_shapes=[pltpu.VMEM((NBR_LEN, columns), BF16)],
        compiler_params=params(SELF_MIB),
        cost_estimate=cost(1000000000 * count, 8 * query.size, query.size),
        name="self_attention",
    )(in_hbm(query), in_hbm(key), in_hbm(value))


def squares_kernel(rows_ref, own_ref, squares_ref):
    for n in range(NEIGHBOURS):
        total = jnp.zeros((NBR_LEN, HEAD_DIM), F32)
        for head in range(rows_ref.shape[1] // HEAD_DIM):
            wide = rows_ref[n * NBR_LEN:(n + 1) * NBR_LEN, columns_of(head)].astype(F32)
            total = total + wide * wide
        squares_ref[n:n + 1, :] = lanes_of(total)
    squares_ref[NEIGHBOURS:, :] = own_ref[...]


def squares_above(rows, own):
    vmem = pl.BlockSpec(memory_space=pltpu.VMEM)
    return pl.pallas_call(
        squares_kernel,
        out_shape=jax.ShapeDtypeStruct((NEIGHBOURS + own.shape[0], NBR_LEN), F32),
        in_specs=[vmem, vmem],
        out_specs=vmem,
        compiler_params=params(SMALL_MIB),
        cost_estimate=cost(1000000000, 2 * rows.size),
        name="row_squares",
    )(rows, own)


def summed(refs, at):
    return functools.reduce(lambda a, b: a + b, [ref[at, :] for ref in refs])


def cross_kernel(full_width, came_ref, rest_ref, got_ref, *refs):
    parts, (out_ref, squares_ref, self_ref) = refs[:-3], refs[-3:]
    step = pl.program_id(0)

    came_steps = NEIGHBOURS * NBR_LEN // self_ref.shape[0]

    @pl.when(step < came_steps)
    def _():
        self_ref[...] = came_ref[...]

    @pl.when(step >= came_steps)
    def _():
        self_ref[...] = rest_ref[...]

    here = self_ref.shape[0] // NBR_LEN
    heads = self_ref.shape[1] // HEAD_DIM
    each = [(i, h) for i in range(here) for h in range(heads)]
    rows_of = [slice(i * NBR_LEN, (i + 1) * NBR_LEN) for i in range(here)]
    at = [columns_of(head) for head in range(heads)]
    scales = [
        lax.rsqrt(summed(parts, pl.ds(step * here + i, 1)) / full_width + EPSILON) * SCALE2
        for i in range(here)
    ]

    def whole(kv, i, h):
        slot = slice(i * HALF, (i + 1) * HALF)
        return jnp.concatenate(
            [got_ref[(2 * kv + half) * heads + h, slot, :] for half in range(2)], axis=0
        )

    scores = [dot(whole(0, i, h), self_ref[rows_of[i], at[h]], (1, 1)) for i, h in each]
    weights = [softmax_down(score, scales[i]) for score, (i, h) in zip(scores, each)]
    sums = [dot(weight, whole(1, i, h), (0, 0)) for weight, (i, h) in zip(weights, each)]
    totals = [jnp.zeros((NBR_LEN, HEAD_DIM), F32) for _ in range(here)]
    for crossed, (i, h) in zip(sums, each):
        own = self_ref[rows_of[i], at[h]].astype(F32)
        rows = (own + crossed.astype(BF16).astype(F32)).astype(BF16)
        out_ref[rows_of[i], at[h]] = rows
        wide = rows.astype(F32)
        totals[i] = totals[i] + wide * wide
    for i in range(here):
        squares_ref[pl.ds(step * here + i, 1), :] = lanes_of(totals[i])


def cross_attention(came, rest, got, parts, full_width, here=NEIGHBOURS):
    columns = came.shape[1]
    count = SEG_DEV * NEIGHBOURS
    rows = count * NBR_LEN
    first = NEIGHBOURS // here
    block = (here * NBR_LEN, columns)
    sums = pl.BlockSpec((count, NBR_LEN), lambda n: (0, 0))
    return pl.pallas_call(
        functools.partial(cross_kernel, full_width),
        grid=(count // here,),
        out_shape=(
            jax.ShapeDtypeStruct((rows, columns), BF16),
            jax.ShapeDtypeStruct((count, NBR_LEN), F32),
        ),
        in_specs=[
            pl.BlockSpec(block, lambda n: (jnp.minimum(n, first - 1), 0)),
            pl.BlockSpec(block, lambda n: (jnp.maximum(n - first, 0), 0)),
            pl.BlockSpec((got.shape[0], here * HALF, HEAD_DIM), lambda n: (0, n, 0)),
        ]
        + [sums] * len(parts),
        out_specs=(pl.BlockSpec(block, lambda n: (n, 0)), sums),
        scratch_shapes=[pltpu.VMEM(block, BF16)],
        compiler_params=params(SMALL_MIB),
        cost_estimate=cost(1000000000 * count, 6 * rows * columns, rows * columns // 2),
        name="cross_attention",
    )(came, rest, got, *parts)


def decode_kernel(full_width, place_ref, query_ref, prior_ref, *refs):
    parts, out_ref = refs[:-1], refs[-1]
    step = pl.program_id(0)
    panel = NEIGHBOURS * NBR_LEN
    here = query_ref.shape[0] // SEG_LEN
    each = [(i, h) for i in range(here) for h in range(query_ref.shape[1] // HEAD_DIM)]
    asks = [slice(i * SEG_LEN, (i + 1) * SEG_LEN) for i in range(here)]
    reads = [slice(i * panel, (i + 1) * panel) for i in range(here)]

    def scale_of(i):
        first = (step * here + i) * NEIGHBOURS
        totals = [summed(parts, pl.ds(first + n, 1)) for n in range(NEIGHBOURS)]
        return lax.rsqrt(jnp.concatenate(totals, axis=1) / full_width + EPSILON) * SCALE2

    scales = [scale_of(i) for i in range(here)]
    empty = (step == 0) & (place_ref[0] == 0)
    scores = [dot(query_ref[asks[i], columns_of(h)], prior_ref[reads[i], columns_of(h)], (1, 1)) for i, h in each]
    weights = [softmax_across(score * scales[i]) for score, (i, h) in zip(scores, each)]
    for weight, (i, h) in zip(weights, each):
        rows = dot(weight, prior_ref[reads[i], columns_of(h)], (1, 0))
        if i == 0:
            rows = jnp.where(empty, 0.0, rows)
        out_ref[asks[i], columns_of(h)] = rows.astype(BF16)


def decode(place, query, prior, parts, full_width, here=2):
    columns = query.shape[1]
    panel = NEIGHBOURS * NBR_LEN
    query_block = pl.BlockSpec((here * SEG_LEN, columns), lambda u: (u, 0))
    sums = pl.BlockSpec(parts[0].shape, lambda u: (0, 0))
    return pl.pallas_call(
        functools.partial(decode_kernel, full_width),
        grid=(SEG_DEV // here,),
        out_shape=jax.ShapeDtypeStruct(query.shape, BF16),
        in_specs=[
            pl.BlockSpec(memory_space=pltpu.SMEM),
            query_block,
            pl.BlockSpec((here * panel, columns), lambda u: (u, 0)),
        ]
        + [sums] * len(parts),
        out_specs=query_block,
        compiler_params=params(SMALL_MIB),
        cost_estimate=cost(4000000000, 4 * query.size + 2 * prior.size, query.size * 2),
        name="decode",
    )(place, query, prior, *parts)


def over_heads(part):
    heads = lax.axis_size("head")
    return [part] + [
        lax.ppermute(part, "head", [(i, (i + step) % heads) for i in range(heads)])
        for step in range(1, heads)
    ]


def from_behind(part):
    devices = lax.axis_size("span")
    return lax.ppermute(part, "span", [(i, i + 1) for i in range(devices - 1)])


def exchange(x):
    return lax.all_to_all(x, "span", split_axis=0, concat_axis=0, tiled=True)


def body(
    neighbour_query,
    neighbour_key,
    neighbour_value,
    segment_key,
    segment_value,
    decoder_query,
    sources,
):
    columns = neighbour_query.shape[1]
    full_width = columns * lax.axis_size("head")
    per_device = SEG_DEV * NEIGHBOURS
    place = lax.axis_index("span").astype(jnp.int32).reshape(1)
    sources, place = lax.optimization_barrier((sources, place))
    table = exchange(pack(sources, segment_key, segment_value))
    rest, panel, rest_squares = self_attention(neighbour_query, neighbour_key, neighbour_value)
    came = from_behind(panel)
    table, rest_squares = lax.optimization_barrier((table, rest_squares))
    named = table[:, SEG_DEV * HALF, :per_device].astype(jnp.int32)
    got = exchange(pick(named, table))
    parts = over_heads(squares_above(came, rest_squares))
    encoded, squares = cross_attention(came, in_hbm(rest), got, parts, full_width)
    return decode(place, decoder_query, encoded, over_heads(squares), full_width)


def solution(mesh):
    placed = (
        P("span", "head"),
        P("span", "head"),
        P("span", "head"),
        P("span", "head"),
        P("span", "head"),
        P("span", "head"),
        P("span", None),
    )
    return jax.shard_map(
        body, mesh=mesh, in_specs=placed, out_specs=P("span", "head"), check_vma=False
    )
```

```python
import functools

import jax
import jax.numpy as jnp
from jax import lax
from jax.experimental import pallas as pl
from jax.experimental.pallas import tpu as pltpu
from jax.sharding import PartitionSpec as P


HEAD_DIM = 128
SEG_LEN = 64
NBR_LEN = 128
NEIGHBOURS = 2
SEG_DEV = 4

EPSILON = 1e-06
LOG2E = 1.4426950408889634
SCALE2 = HEAD_DIM ** (-0.5) * LOG2E
HALF = SEG_LEN // 2
TAIL = 8
AT_ONCE = 2
PACK_MIB = 60
SELF_MIB = 24
PICK_MIB = 24
SMALL_MIB = 24

F32 = jnp.float32
BF16 = jnp.bfloat16


def dot(a, b, contract):
    return lax.dot_general(a, b, ((contract[:1], contract[1:]), ((), ())), preferred_element_type=F32)


def cost(flops, moved, exps=0):
    return pl.CostEstimate(flops=flops, bytes_accessed=moved, transcendentals=exps)


def params(mib):
    return pltpu.CompilerParams(vmem_limit_bytes=mib * 1024 * 1024)


def in_hbm(x):
    return pltpu.with_memory_space_constraint(x, pltpu.HBM)


def pack_kernel(sources_ref, key_ref, value_ref, out_ref, rows_ref, packed_ref, in_sems, out_sems):
    heads = key_ref.shape[1] // HEAD_DIM

    def into(kv, seg):
        at = pl.ds(seg * SEG_LEN, SEG_LEN)
        ref = (key_ref, value_ref)[kv]
        return pltpu.make_async_copy(ref.at[at, :], rows_ref.at[kv, at, :], in_sems.at[kv, seg])

    def out_of(seg):
        at = pl.ds(seg * HALF, HALF + TAIL if seg == SEG_DEV - 1 else HALF)
        return pltpu.make_async_copy(packed_ref.at[:, at, :], out_ref.at[:, at, :], out_sems.at[seg])

    for seg in range(SEG_DEV):
        for kv in range(2):
            into(kv, seg).start()
    lane = lax.broadcasted_iota(jnp.int32, (TAIL, HEAD_DIM), 1)
    tail = jnp.zeros((TAIL, HEAD_DIM), F32)
    for i in range(SEG_DEV * NEIGHBOURS):
        named = sources_ref[i % NEIGHBOURS, i // NEIGHBOURS].astype(F32)
        tail = jnp.where(lane == i, named, tail)
    tail = tail.astype(BF16)
    for stripe in range(4 * heads):
        packed_ref[stripe, SEG_DEV * HALF:SEG_DEV * HALF + TAIL, :] = tail
    for seg in range(SEG_DEV):
        for kv in range(2):
            into(kv, seg).wait()
            for half in range(2):
                row = seg * SEG_LEN + half * HALF
                for head in range(heads):
                    packed_ref[(kv * 2 + half) * heads + head, seg * HALF:(seg + 1) * HALF, :] = rows_ref[
                        kv, row:row + HALF, head * HEAD_DIM:(head + 1) * HEAD_DIM
                    ]
        out_of(seg).start()
    for seg in range(SEG_DEV):
        out_of(seg).wait()


def pack(sources, segment_key, segment_value):
    rows, columns = segment_key.shape
    shape = (4 * columns // HEAD_DIM, SEG_DEV * HALF + TAIL, HEAD_DIM)
    hbm = pl.BlockSpec(memory_space=pl.ANY)
    return pl.pallas_call(
        pack_kernel,
        out_shape=jax.ShapeDtypeStruct(shape, BF16),
        in_specs=[pl.BlockSpec(memory_space=pltpu.SMEM), hbm, hbm],
        out_specs=hbm,
        scratch_shapes=[
            pltpu.VMEM((2, rows, columns), BF16),
            pltpu.VMEM(shape, BF16),
            pltpu.SemaphoreType.DMA((2, SEG_DEV)),
            pltpu.SemaphoreType.DMA((SEG_DEV,)),
        ],
        compiler_params=params(PACK_MIB),
        cost_estimate=cost(1000000, 2 * 2 * segment_key.size * 2),
        name="pack_stripes",
    )(sources.T, segment_key, segment_value)


def pick_kernel(named_ref, table_ref, out_ref, picked_ref, sems):
    devices = table_ref.shape[0]
    groups = sems.shape[0]
    here = devices // groups
    count = SEG_DEV * NEIGHBOURS

    def out_of(group):
        at = pl.ds(group * here, here)
        return pltpu.make_async_copy(picked_ref.at[at], out_ref.at[at], sems.at[group])

    def one(group, carry):
        for step in range(here):
            device = group * here + step
            behind = lax.rem(device + devices - 1, devices)
            for i in range(count):
                if i < NEIGHBOURS:
                    named = named_ref[behind, count - NEIGHBOURS + i]
                else:
                    named = named_ref[device, i - NEIGHBOURS]
                owner = lax.shift_right_logical(named, 2)
                within = lax.bitwise_and(named, SEG_DEV - 1)
                start = pl.multiple_of(within * HALF, HALF)
                picked_ref[device, i * HALF:(i + 1) * HALF, :] = table_ref[owner, pl.ds(start, HALF), :]
        out_of(group).start()
        return carry

    lax.fori_loop(0, groups, one, 0)
    for group in range(groups):
        out_of(group).wait()


def pick(named, table):
    devices = table.shape[0]
    shape = (devices, SEG_DEV * NEIGHBOURS * HALF, HEAD_DIM)
    groups = 8
    return pl.pallas_call(
        pick_kernel,
        out_shape=jax.ShapeDtypeStruct(shape, BF16),
        in_specs=[pl.BlockSpec(memory_space=pltpu.SMEM), pl.BlockSpec(memory_space=pltpu.VMEM)],
        out_specs=pl.BlockSpec(memory_space=pl.ANY),
        scratch_shapes=[pltpu.VMEM(shape, BF16), pltpu.SemaphoreType.DMA((groups,))],
        compiler_params=params(PICK_MIB),
        cost_estimate=cost(1000000, 2 * table.size + 2 * devices * shape[1] * HEAD_DIM),
        name="pick_stripes",
    )(named, table)


def lanes_of(square):
    return jnp.sum(square.T, axis=0, keepdims=True)


def columns_of(head):
    return slice(head * HEAD_DIM, (head + 1) * HEAD_DIM)


def softmax_down(scores, scale):
    weights = jnp.exp2((scores - jnp.max(scores, axis=0, keepdims=True)) * scale)
    return (weights * (1.0 / jnp.sum(weights, axis=0, keepdims=True))).astype(BF16)


def softmax_across(scores):
    weights = jnp.exp2(scores - jnp.max(scores, axis=1, keepdims=True))
    return (weights * (1.0 / jnp.sum(weights, axis=1, keepdims=True))).astype(BF16)


def self_kernel(query_ref, key_ref, value_ref, rest_ref, panel_ref, squares_ref, held_ref):
    n = pl.program_id(0)
    last = pl.num_programs(0) - NEIGHBOURS
    heads = range(query_ref.shape[1] // HEAD_DIM)
    at = [columns_of(head) for head in heads]
    scores = [dot(key_ref[:, at[h]], query_ref[:, at[h]], (1, 1)) for h in heads]
    weights = [softmax_down(scores[h], SCALE2) for h in heads]
    sums = [dot(weights[h], value_ref[:, at[h]], (0, 0)) for h in heads]
    total = jnp.zeros((NBR_LEN, HEAD_DIM), F32)
    for h in heads:
        rows = sums[h].astype(BF16)
        held_ref[:, at[h]] = rows
        wide = rows.astype(F32)
        total = total + wide * wide

    @pl.when(n < last)
    def _():
        rest_ref[...] = held_ref[...]
        squares_ref[pl.ds(n, 1), :] = lanes_of(total)

    @pl.when(n >= last)
    def _():
        panel_ref[...] = held_ref[...]


def self_attention(query, key, value):
    columns = query.shape[1]
    count = query.shape[0] // NBR_LEN
    last = count - NEIGHBOURS
    block = pl.BlockSpec((NBR_LEN, columns), lambda n: (n, 0))
    return pl.pallas_call(
        self_kernel,
        grid=(count,),
        out_shape=(
            pltpu.HBM((last * NBR_LEN, columns), BF16),
            pltpu.HBM((NEIGHBOURS * NBR_LEN, columns), BF16),
            jax.ShapeDtypeStruct((last, NBR_LEN), F32),
        ),
        in_specs=[block, block, block],
        out_specs=(
            pl.BlockSpec((NBR_LEN, columns), lambda n: (jnp.minimum(n, last - 1), 0)),
            pl.BlockSpec((NBR_LEN, columns), lambda n: (jnp.maximum(n - last, 0), 0)),
            pl.BlockSpec((last, NBR_LEN), lambda n: (0, 0)),
        ),
        scratch_shapes=[pltpu.VMEM((NBR_LEN, columns), BF16)],
        compiler_params=params(SELF_MIB),
        cost_estimate=cost(1000000000 * count, 8 * query.size, query.size),
        name="self_attention",
    )(in_hbm(query), in_hbm(key), in_hbm(value))


def squares_kernel(rows_ref, own_ref, squares_ref):
    for n in range(NEIGHBOURS):
        total = jnp.zeros((NBR_LEN, HEAD_DIM), F32)
        for head in range(rows_ref.shape[1] // HEAD_DIM):
            wide = rows_ref[n * NBR_LEN:(n + 1) * NBR_LEN, columns_of(head)].astype(F32)
            total = total + wide * wide
        squares_ref[n:n + 1, :] = lanes_of(total)
    squares_ref[NEIGHBOURS:, :] = own_ref[...]


def squares_above(rows, own):
    vmem = pl.BlockSpec(memory_space=pltpu.VMEM)
    return pl.pallas_call(
        squares_kernel,
        out_shape=jax.ShapeDtypeStruct((NEIGHBOURS + own.shape[0], NBR_LEN), F32),
        in_specs=[vmem, vmem],
        out_specs=vmem,
        compiler_params=params(SMALL_MIB),
        cost_estimate=cost(1000000000, 2 * rows.size),
        name="row_squares",
    )(rows, own)


def summed(refs, at):
    return functools.reduce(lambda a, b: a + b, [ref[at, :] for ref in refs])


def cross_kernel(full_width, came_ref, rest_ref, got_ref, *refs):
    parts, (out_ref, squares_ref, rest_rows, sems) = refs[:-4], refs[-4:]
    panel = NEIGHBOURS * NBR_LEN
    heads = came_ref.shape[1] // HEAD_DIM

    def into(seg):
        at = pl.ds((seg - 1) * panel, panel)
        return pltpu.make_async_copy(rest_ref.at[at, :], rest_rows.at[at, :], sems.at[seg - 1])

    for seg in range(1, SEG_DEV):
        into(seg).start()
    for seg in range(SEG_DEV):
        if seg > 0:
            into(seg).wait()
        each = [(seg * NEIGHBOURS + i, h) for i in range(NEIGHBOURS) for h in range(heads)]

        def own(n, h):
            first = n * NBR_LEN - (panel if seg > 0 else 0)
            ref = rest_rows if seg > 0 else came_ref
            return ref[first:first + NBR_LEN, columns_of(h)]

        def whole(kv, n, h):
            slot = slice(n * HALF, (n + 1) * HALF)
            return jnp.concatenate(
                [got_ref[(2 * kv + half) * heads + h, slot, :] for half in range(2)], axis=0
            )

        total = summed(parts, slice(seg * NEIGHBOURS, (seg + 1) * NEIGHBOURS))
        scale = lax.rsqrt(total / full_width + EPSILON) * SCALE2
        scores = [dot(whole(0, n, h), own(n, h), (1, 1)) for n, h in each]
        weights = [
            softmax_down(score, scale[n % NEIGHBOURS:n % NEIGHBOURS + 1, :])
            for score, (n, h) in zip(scores, each)
        ]
        sums = [dot(weight, whole(1, n, h), (0, 0)) for weight, (n, h) in zip(weights, each)]
        squares = {n: jnp.zeros((NBR_LEN, HEAD_DIM), F32) for n, _ in each}
        for crossed, (n, h) in zip(sums, each):
            rows = (own(n, h).astype(F32) + crossed.astype(BF16).astype(F32)).astype(BF16)
            out_ref[n * NBR_LEN:(n + 1) * NBR_LEN, columns_of(h)] = rows
            wide = rows.astype(F32)
            squares[n] = squares[n] + wide * wide
        for n in squares:
            squares_ref[n:n + 1, :] = lanes_of(squares[n])


def cross_attention(came, rest, got, parts, full_width):
    columns = came.shape[1]
    count = SEG_DEV * NEIGHBOURS
    rows = count * NBR_LEN
    vmem = pl.BlockSpec(memory_space=pltpu.VMEM)
    return pl.pallas_call(
        functools.partial(cross_kernel, full_width),
        out_shape=(
            jax.ShapeDtypeStruct((rows, columns), BF16),
            jax.ShapeDtypeStruct((count, NBR_LEN), F32),
        ),
        in_specs=[vmem, pl.BlockSpec(memory_space=pl.ANY), vmem] + [vmem] * len(parts),
        out_specs=(vmem, vmem),
        scratch_shapes=[pltpu.VMEM(rest.shape, BF16), pltpu.SemaphoreType.DMA((SEG_DEV - 1,))],
        compiler_params=params(SMALL_MIB),
        cost_estimate=cost(1000000000 * count, 6 * rows * columns, rows * columns // 2),
        name="cross_attention",
    )(came, in_hbm(rest), got, *parts)


def decode_kernel(full_width, place_ref, query_ref, prior_ref, *refs):
    parts, (out_ref, out_rows, sems) = refs[:-3], refs[-3:]
    panel = NEIGHBOURS * NBR_LEN
    heads = query_ref.shape[1] // HEAD_DIM
    empty = place_ref[0] == 0

    def out_of(group):
        at = pl.ds(group * AT_ONCE * SEG_LEN, AT_ONCE * SEG_LEN)
        return pltpu.make_async_copy(out_rows.at[at, :], out_ref.at[at, :], sems.at[group])

    totals = summed(parts, slice(None))
    scales = lax.rsqrt(totals / full_width + EPSILON) * SCALE2
    for group in range(SEG_DEV // AT_ONCE):
        each = [(group * AT_ONCE + i, h) for i in range(AT_ONCE) for h in range(heads)]
        scale = {
            u: jnp.concatenate(
                [scales[n:n + 1, :] for n in range(u * NEIGHBOURS, (u + 1) * NEIGHBOURS)], axis=1
            )
            for u, _ in each
        }

        def prior(u, h):
            return prior_ref[u * panel:(u + 1) * panel, columns_of(h)]

        scores = [
            dot(query_ref[u * SEG_LEN:(u + 1) * SEG_LEN, columns_of(h)], prior(u, h), (1, 1))
            for u, h in each
        ]
        weights = [softmax_across(score * scale[u]) for score, (u, h) in zip(scores, each)]
        for weight, (u, h) in zip(weights, each):
            rows = dot(weight, prior(u, h), (1, 0))
            if u == 0:
                rows = jnp.where(empty, 0.0, rows)
            out_rows[u * SEG_LEN:(u + 1) * SEG_LEN, columns_of(h)] = rows.astype(BF16)
        out_of(group).start()
    for group in range(SEG_DEV // AT_ONCE):
        out_of(group).wait()


def decode(place, query, prior, parts, full_width):
    vmem = pl.BlockSpec(memory_space=pltpu.VMEM)
    return pl.pallas_call(
        functools.partial(decode_kernel, full_width),
        out_shape=jax.ShapeDtypeStruct(query.shape, BF16),
        in_specs=[pl.BlockSpec(memory_space=pltpu.SMEM), vmem, vmem] + [vmem] * len(parts),
        out_specs=pl.BlockSpec(memory_space=pl.ANY),
        scratch_shapes=[
            pltpu.VMEM(query.shape, BF16),
            pltpu.SemaphoreType.DMA((SEG_DEV // AT_ONCE,)),
        ],
        compiler_params=params(SMALL_MIB),
        cost_estimate=cost(4000000000, 4 * query.size + 2 * prior.size, query.size * 2),
        name="decode",
    )(place, query, prior, *parts)


def over_heads(part):
    heads = lax.axis_size("head")
    return [part] + [
        lax.ppermute(part, "head", [(i, (i + step) % heads) for i in range(heads)])
        for step in range(1, heads)
    ]


def from_behind(part):
    devices = lax.axis_size("span")
    return lax.ppermute(part, "span", [(i, i + 1) for i in range(devices - 1)])


def exchange(x):
    return lax.all_to_all(x, "span", split_axis=0, concat_axis=0, tiled=True)


def body(
    neighbour_query,
    neighbour_key,
    neighbour_value,
    segment_key,
    segment_value,
    decoder_query,
    sources,
):
    columns = neighbour_query.shape[1]
    full_width = columns * lax.axis_size("head")
    per_device = SEG_DEV * NEIGHBOURS
    place = lax.axis_index("span").astype(jnp.int32).reshape(1)
    sources, place = lax.optimization_barrier((sources, place))
    table = exchange(pack(sources, segment_key, segment_value))
    rest, panel, rest_squares = self_attention(neighbour_query, neighbour_key, neighbour_value)
    came = from_behind(panel)
    table, rest_squares = lax.optimization_barrier((table, rest_squares))
    named = table[:, SEG_DEV * HALF, :per_device].astype(jnp.int32)
    got = exchange(pick(named, table))
    parts = over_heads(squares_above(came, rest_squares))
    encoded, squares = cross_attention(came, rest, got, parts, full_width)
    return decode(place, decoder_query, encoded, over_heads(squares), full_width)


def solution(mesh):
    placed = (
        P("span", "head"),
        P("span", "head"),
        P("span", "head"),
        P("span", "head"),
        P("span", "head"),
        P("span", "head"),
        P("span", None),
    )
    return jax.shard_map(
        body, mesh=mesh, in_specs=placed, out_specs=P("span", "head"), check_vma=False
    )
```

```python
import functools

import jax
import jax.numpy as jnp
from jax import lax
from jax.experimental import pallas as pl
from jax.experimental.pallas import tpu as pltpu
from jax.sharding import PartitionSpec as P


HEAD_DIM = 128
SEG_LEN = 64
NBR_LEN = 128
NEIGHBOURS = 2
SEG_DEV = 4

EPSILON = 1e-06
LOG2E = 1.4426950408889634
SCALE2 = HEAD_DIM ** (-0.5) * LOG2E
HALF = SEG_LEN // 2
TAIL = 8
AT_ONCE = 2
PACK_MIB = 60
SELF_MIB = 24
PICK_MIB = 24
SMALL_MIB = 24

F32 = jnp.float32
BF16 = jnp.bfloat16


def dot(a, b, contract):
    return lax.dot_general(a, b, ((contract[:1], contract[1:]), ((), ())), preferred_element_type=F32)


def cost(flops, moved, exps=0):
    return pl.CostEstimate(flops=flops, bytes_accessed=moved, transcendentals=exps)


def params(mib):
    return pltpu.CompilerParams(vmem_limit_bytes=mib * 1024 * 1024)


def in_hbm(x):
    return pltpu.with_memory_space_constraint(x, pltpu.HBM)


def pack_kernel(sources_ref, key_ref, value_ref, out_ref, rows_ref, packed_ref, listed_ref, in_sems, out_sems, listed_sem):
    heads = key_ref.shape[1] // HEAD_DIM

    def into(kv, seg):
        at = pl.ds(seg * SEG_LEN, SEG_LEN)
        ref = (key_ref, value_ref)[kv]
        return pltpu.make_async_copy(ref.at[at, :], rows_ref.at[kv, at, :], in_sems.at[kv, seg])

    def out_of(seg):
        at = pl.ds(seg * HALF, HALF + TAIL if seg == SEG_DEV - 1 else HALF)
        return pltpu.make_async_copy(packed_ref.at[:, at, :], out_ref.at[:, at, :], out_sems.at[seg])

    listing = pltpu.make_async_copy(sources_ref, listed_ref, listed_sem)
    listing.start()
    for seg in range(SEG_DEV):
        for kv in range(2):
            into(kv, seg).start()
    listing.wait()
    lane = lax.broadcasted_iota(jnp.int32, (TAIL, HEAD_DIM), 1)
    tail = jnp.zeros((TAIL, HEAD_DIM), F32)
    for i in range(SEG_DEV * NEIGHBOURS):
        named = listed_ref[i % NEIGHBOURS, i // NEIGHBOURS].astype(F32)
        tail = jnp.where(lane == i, named, tail)
    tail = tail.astype(BF16)
    for stripe in range(4 * heads):
        packed_ref[stripe, SEG_DEV * HALF:SEG_DEV * HALF + TAIL, :] = tail
    for seg in range(SEG_DEV):
        for kv in range(2):
            into(kv, seg).wait()
            for half in range(2):
                row = seg * SEG_LEN + half * HALF
                for head in range(heads):
                    packed_ref[(kv * 2 + half) * heads + head, seg * HALF:(seg + 1) * HALF, :] = rows_ref[
                        kv, row:row + HALF, head * HEAD_DIM:(head + 1) * HEAD_DIM
                    ]
        out_of(seg).start()
    for seg in range(SEG_DEV):
        out_of(seg).wait()


def pack(sources, segment_key, segment_value):
    rows, columns = segment_key.shape
    shape = (4 * columns // HEAD_DIM, SEG_DEV * HALF + TAIL, HEAD_DIM)
    hbm = pl.BlockSpec(memory_space=pl.ANY)
    return pl.pallas_call(
        pack_kernel,
        out_shape=jax.ShapeDtypeStruct(shape, BF16),
        in_specs=[hbm, hbm, hbm],
        out_specs=hbm,
        scratch_shapes=[
            pltpu.VMEM((2, rows, columns), BF16),
            pltpu.VMEM(shape, BF16),
            pltpu.SMEM((NEIGHBOURS, SEG_DEV), jnp.int32),
            pltpu.SemaphoreType.DMA((2, SEG_DEV)),
            pltpu.SemaphoreType.DMA((SEG_DEV,)),
            pltpu.SemaphoreType.DMA,
        ],
        compiler_params=params(PACK_MIB),
        cost_estimate=cost(1000000, 2 * 2 * segment_key.size * 2),
        name="pack_stripes",
    )(sources.T, segment_key, segment_value)


def pick_kernel(named_ref, table_ref, out_ref, picked_ref, sems):
    devices, long, _ = table_ref.shape
    rows_ref = table_ref.reshape(devices * long, HEAD_DIM)
    groups = sems.shape[0]
    here = devices // groups
    count = SEG_DEV * NEIGHBOURS

    def out_of(group):
        at = pl.ds(group * here, here)
        return pltpu.make_async_copy(picked_ref.at[at], out_ref.at[at], sems.at[group])

    def one(group, carry):
        for step in range(here):
            device = group * here + step
            behind = lax.rem(device + devices - 1, devices)
            for i in range(count):
                if i < NEIGHBOURS:
                    named = named_ref[behind, count - NEIGHBOURS + i]
                else:
                    named = named_ref[device, i - NEIGHBOURS]
                start = pl.multiple_of(named * HALF + lax.shift_right_logical(named, 2) * TAIL, TAIL)
                picked_ref[device, i * HALF:(i + 1) * HALF, :] = rows_ref[pl.ds(start, HALF), :]
        out_of(group).start()
        return carry

    lax.fori_loop(0, groups, one, 0)
    for group in range(groups):
        out_of(group).wait()


def pick(named, table):
    devices = table.shape[0]
    shape = (devices, SEG_DEV * NEIGHBOURS * HALF, HEAD_DIM)
    groups = 8
    return pl.pallas_call(
        pick_kernel,
        out_shape=jax.ShapeDtypeStruct(shape, BF16),
        in_specs=[pl.BlockSpec(memory_space=pltpu.SMEM), pl.BlockSpec(memory_space=pltpu.VMEM)],
        out_specs=pl.BlockSpec(memory_space=pl.ANY),
        scratch_shapes=[pltpu.VMEM(shape, BF16), pltpu.SemaphoreType.DMA((groups,))],
        compiler_params=params(PICK_MIB),
        cost_estimate=cost(1000000, 2 * table.size + 2 * devices * shape[1] * HEAD_DIM),
        name="pick_stripes",
    )(named, table)


def lanes_of(square):
    return jnp.sum(square.T, axis=0, keepdims=True)


def columns_of(head):
    return slice(head * HEAD_DIM, (head + 1) * HEAD_DIM)


def softmax_down(scores, scale):
    weights = jnp.exp2((scores - jnp.max(scores, axis=0, keepdims=True)) * scale)
    return (weights * (1.0 / jnp.sum(weights, axis=0, keepdims=True))).astype(BF16)


def softmax_across(scores):
    weights = jnp.exp2(scores - jnp.max(scores, axis=1, keepdims=True))
    return (weights * (1.0 / jnp.sum(weights, axis=1, keepdims=True))).astype(BF16)


def self_kernel(query_ref, key_ref, value_ref, rest_ref, panel_ref, squares_ref, held_ref):
    n = pl.program_id(0)
    last = pl.num_programs(0) - NEIGHBOURS
    heads = range(query_ref.shape[1] // HEAD_DIM)
    at = [columns_of(head) for head in heads]
    scores = [dot(key_ref[:, at[h]], query_ref[:, at[h]], (1, 1)) for h in heads]
    weights = [softmax_down(scores[h], SCALE2) for h in heads]
    sums = [dot(weights[h], value_ref[:, at[h]], (0, 0)) for h in heads]
    total = jnp.zeros((NBR_LEN, HEAD_DIM), F32)
    for h in heads:
        rows = sums[h].astype(BF16)
        held_ref[:, at[h]] = rows
        wide = rows.astype(F32)
        total = total + wide * wide

    @pl.when(n < last)
    def _():
        rest_ref[...] = held_ref[...]
        squares_ref[pl.ds(n, 1), :] = lanes_of(total)

    @pl.when(n >= last)
    def _():
        panel_ref[...] = held_ref[...]


def self_attention(query, key, value):
    columns = query.shape[1]
    count = query.shape[0] // NBR_LEN
    last = count - NEIGHBOURS
    block = pl.BlockSpec((NBR_LEN, columns), lambda n: (n, 0))
    return pl.pallas_call(
        self_kernel,
        grid=(count,),
        out_shape=(
            pltpu.HBM((last * NBR_LEN, columns), BF16),
            pltpu.HBM((NEIGHBOURS * NBR_LEN, columns), BF16),
            jax.ShapeDtypeStruct((last, NBR_LEN), F32),
        ),
        in_specs=[block, block, block],
        out_specs=(
            pl.BlockSpec((NBR_LEN, columns), lambda n: (jnp.minimum(n, last - 1), 0)),
            pl.BlockSpec((NBR_LEN, columns), lambda n: (jnp.maximum(n - last, 0), 0)),
            pl.BlockSpec((last, NBR_LEN), lambda n: (0, 0)),
        ),
        scratch_shapes=[pltpu.VMEM((NBR_LEN, columns), BF16)],
        compiler_params=params(SELF_MIB),
        cost_estimate=cost(1000000000 * count, 8 * query.size, query.size),
        name="self_attention",
    )(in_hbm(query), in_hbm(key), in_hbm(value))


def squares_kernel(rows_ref, own_ref, squares_ref):
    for n in range(NEIGHBOURS):
        total = jnp.zeros((NBR_LEN, HEAD_DIM), F32)
        for head in range(rows_ref.shape[1] // HEAD_DIM):
            wide = rows_ref[n * NBR_LEN:(n + 1) * NBR_LEN, columns_of(head)].astype(F32)
            total = total + wide * wide
        squares_ref[n:n + 1, :] = lanes_of(total)
    squares_ref[NEIGHBOURS:, :] = own_ref[...]


def squares_above(rows, own):
    vmem = pl.BlockSpec(memory_space=pltpu.VMEM)
    return pl.pallas_call(
        squares_kernel,
        out_shape=jax.ShapeDtypeStruct((NEIGHBOURS + own.shape[0], NBR_LEN), F32),
        in_specs=[vmem, vmem],
        out_specs=vmem,
        compiler_params=params(SMALL_MIB),
        cost_estimate=cost(1000000000, 2 * rows.size),
        name="row_squares",
    )(rows, own)


def summed(refs, at):
    return functools.reduce(lambda a, b: a + b, [ref[at, :] for ref in refs])


def cross_kernel(full_width, came_ref, rest_ref, got_ref, *refs):
    parts, (out_ref, squares_ref, rest_rows, sems) = refs[:-4], refs[-4:]
    panel = NEIGHBOURS * NBR_LEN
    heads = came_ref.shape[1] // HEAD_DIM

    def into(seg):
        at = pl.ds((seg - 1) * panel, panel)
        return pltpu.make_async_copy(rest_ref.at[at, :], rest_rows.at[at, :], sems.at[seg - 1])

    for seg in range(1, SEG_DEV):
        into(seg).start()
    for seg in range(SEG_DEV):
        if seg == 1:
            for behind in range(1, SEG_DEV):
                into(behind).wait()
        each = [(seg * NEIGHBOURS + i, h) for i in range(NEIGHBOURS) for h in range(heads)]

        def own(n, h):
            first = n * NBR_LEN - (panel if seg > 0 else 0)
            ref = rest_rows if seg > 0 else came_ref
            return ref[first:first + NBR_LEN, columns_of(h)]

        def whole(kv, n, h):
            slot = slice(n * HALF, (n + 1) * HALF)
            return jnp.concatenate(
                [got_ref[(2 * kv + half) * heads + h, slot, :] for half in range(2)], axis=0
            )

        total = summed(parts, slice(seg * NEIGHBOURS, (seg + 1) * NEIGHBOURS))
        scale = lax.rsqrt(total / full_width + EPSILON) * SCALE2
        scores = [dot(whole(0, n, h), own(n, h), (1, 1)) for n, h in each]
        weights = [
            softmax_down(score, scale[n % NEIGHBOURS:n % NEIGHBOURS + 1, :])
            for score, (n, h) in zip(scores, each)
        ]
        sums = [dot(weight, whole(1, n, h), (0, 0)) for weight, (n, h) in zip(weights, each)]
        squares = {n: jnp.zeros((NBR_LEN, HEAD_DIM), F32) for n, _ in each}
        for crossed, (n, h) in zip(sums, each):
            rows = (own(n, h).astype(F32) + crossed.astype(BF16).astype(F32)).astype(BF16)
            out_ref[n * NBR_LEN:(n + 1) * NBR_LEN, columns_of(h)] = rows
            wide = rows.astype(F32)
            squares[n] = squares[n] + wide * wide
        for n in squares:
            squares_ref[n:n + 1, :] = lanes_of(squares[n])


def cross_attention(came, rest, got, parts, full_width):
    columns = came.shape[1]
    count = SEG_DEV * NEIGHBOURS
    rows = count * NBR_LEN
    vmem = pl.BlockSpec(memory_space=pltpu.VMEM)
    return pl.pallas_call(
        functools.partial(cross_kernel, full_width),
        out_shape=(
            jax.ShapeDtypeStruct((rows, columns), BF16),
            jax.ShapeDtypeStruct((count, NBR_LEN), F32),
        ),
        in_specs=[vmem, pl.BlockSpec(memory_space=pl.ANY), vmem] + [vmem] * len(parts),
        out_specs=(vmem, vmem),
        scratch_shapes=[pltpu.VMEM(rest.shape, BF16), pltpu.SemaphoreType.DMA((SEG_DEV - 1,))],
        compiler_params=params(SMALL_MIB),
        cost_estimate=cost(1000000000 * count, 6 * rows * columns, rows * columns // 2),
        name="cross_attention",
    )(came, in_hbm(rest), got, *parts)


def decode_kernel(full_width, query_ref, prior_ref, *refs):
    parts, (out_ref, out_rows, sems) = refs[:-3], refs[-3:]
    panel = NEIGHBOURS * NBR_LEN
    heads = query_ref.shape[1] // HEAD_DIM
    empty = lax.axis_index("span") == 0

    def out_of(group):
        at = pl.ds(group * AT_ONCE * SEG_LEN, AT_ONCE * SEG_LEN)
        return pltpu.make_async_copy(out_rows.at[at, :], out_ref.at[at, :], sems.at[group])

    totals = summed(parts, slice(None))
    scales = lax.rsqrt(totals / full_width + EPSILON) * SCALE2
    for group in range(SEG_DEV // AT_ONCE):
        each = [(group * AT_ONCE + i, h) for i in range(AT_ONCE) for h in range(heads)]
        scale = {
            u: jnp.concatenate(
                [scales[n:n + 1, :] for n in range(u * NEIGHBOURS, (u + 1) * NEIGHBOURS)], axis=1
            )
            for u, _ in each
        }

        def prior(u, h):
            return prior_ref[u * panel:(u + 1) * panel, columns_of(h)]

        scores = [
            dot(query_ref[u * SEG_LEN:(u + 1) * SEG_LEN, columns_of(h)], prior(u, h), (1, 1))
            for u, h in each
        ]
        weights = [softmax_across(score * scale[u]) for score, (u, h) in zip(scores, each)]
        for weight, (u, h) in zip(weights, each):
            rows = dot(weight, prior(u, h), (1, 0))
            if u == 0:
                rows = jnp.where(empty, 0.0, rows)
            out_rows[u * SEG_LEN:(u + 1) * SEG_LEN, columns_of(h)] = rows.astype(BF16)
        out_of(group).start()
    for group in range(SEG_DEV // AT_ONCE):
        out_of(group).wait()


def decode(query, prior, parts, full_width):
    vmem = pl.BlockSpec(memory_space=pltpu.VMEM)
    return pl.pallas_call(
        functools.partial(decode_kernel, full_width),
        out_shape=jax.ShapeDtypeStruct(query.shape, BF16),
        in_specs=[vmem, vmem] + [vmem] * len(parts),
        out_specs=pl.BlockSpec(memory_space=pl.ANY),
        scratch_shapes=[
            pltpu.VMEM(query.shape, BF16),
            pltpu.SemaphoreType.DMA((SEG_DEV // AT_ONCE,)),
        ],
        compiler_params=params(SMALL_MIB),
        cost_estimate=cost(4000000000, 4 * query.size + 2 * prior.size, query.size * 2),
        name="decode",
    )(query, prior, *parts)


def over_heads(part):
    heads = lax.axis_size("head")
    return [part] + [
        lax.ppermute(part, "head", [(i, (i + step) % heads) for i in range(heads)])
        for step in (1, 3, 2)
    ]


def from_behind(part):
    devices = lax.axis_size("span")
    return lax.ppermute(part, "span", [(i, i + 1) for i in range(devices - 1)])


def exchange(x):
    return lax.all_to_all(x, "span", split_axis=0, concat_axis=0, tiled=True)


def body(
    neighbour_query,
    neighbour_key,
    neighbour_value,
    segment_key,
    segment_value,
    decoder_query,
    sources,
):
    columns = neighbour_query.shape[1]
    full_width = columns * lax.axis_size("head")
    per_device = SEG_DEV * NEIGHBOURS
    table = exchange(pack(sources, segment_key, segment_value))
    rest, panel, rest_squares = self_attention(neighbour_query, neighbour_key, neighbour_value)
    came = from_behind(panel)
    table, rest_squares = lax.optimization_barrier((table, rest_squares))
    named = table[:, SEG_DEV * HALF, :per_device].astype(jnp.int32)
    got = exchange(pick(named, table))
    parts = over_heads(squares_above(came, rest_squares))
    encoded, squares = cross_attention(came, rest, got, parts, full_width)
    return decode(decoder_query, encoded, over_heads(squares), full_width)


def solution(mesh):
    placed = (
        P("span", "head"),
        P("span", "head"),
        P("span", "head"),
        P("span", "head"),
        P("span", "head"),
        P("span", "head"),
        P("span", None),
    )
    return jax.shard_map(
        body, mesh=mesh, in_specs=placed, out_specs=P("span", "head"), check_vma=False
    )
```
